256 devices in a mesh: dp: 64 (over x, z_lo, y, core), sub: 4 (over z_hi).
Axes of the slice: x: 4, y: 4, z: 8 (z_hi: 4, z_lo: 2; z = z_hi * 2 + z_lo), core: 2. Of those that a mesh axis runs over, the one named last changes fastest.
Arguments:
- queries: float32 [16384, 1024], P(('dp', 'sub')), may hold values from -8 to 8
- passages: float32 [16384, 1024], P(('dp', 'sub')), may hold values from -8 to 8
- positives: int32 [16384], P(('dp', 'sub')), may hold values from 0 to 16383, each once
Outputs:
- losses: float32 [16384], P(('dp', 'sub'))
- query_grads: float32 [16384, 1024], P(('dp', 'sub'))
- passage_grads: float32 [16384, 1024], P(('dp', 'sub'))
The draws below stay inside these ranges and needn't reach their ends.
All inputs are finite; a program needn't handle non-finite values.
Results may differ from the reference program's by a relative error of at most 0.00185.
The reference program's roundings to bfloat16 on the way count: a program that leaves them out, or rounds other values in their place, can miss the bound.
Values may be sent and summed in bfloat16 or wider, within the bound.
A program may use at most 128 MiB of HBM per device.

```python
import math
import jax
import jax.numpy as jnp
from jax import lax

D = 1024
BATCH = 16384


def embedding_pair(key):
    base = jax.random.fold_in(key, 41)
    streams = jax.random.split(base, 2)
    spread = (0.115 / math.sqrt(D)) ** 0.5
    queries = spread * jax.random.normal(streams[0], (BATCH, D), jnp.float32)
    passages = spread * jax.random.normal(streams[1], (BATCH, D), jnp.float32)
    return (jnp.clip(queries, -8.0, 8.0), jnp.clip(passages, -8.0, 8.0))


def draw_queries(key, part):
    return embedding_pair(key)[0]


def draw_passages(key, part):
    return embedding_pair(key)[1]


def setup_inputs(seed: int = 0) -> dict:
    splits = jax.random.split(jax.random.key(seed), 4)
    queries = draw_queries(jax.random.fold_in(splits[3], 71), 0)
    passages = draw_passages(jax.random.fold_in(splits[3], 71), 0)
    positives = jax.random.permutation(splits[2], BATCH).astype(jnp.int32)
    return {"queries": queries, "passages": passages, "positives": positives}


logit_scale = 20.0


def widen(values):
    return lax.optimization_barrier(values.astype(jnp.bfloat16)).astype(jnp.float32)


def reference(queries, passages, positives):
    query_wide = widen(queries)
    passage_wide = widen(passages)
    height = math.gcd(BATCH, 512)
    column_ids = jnp.arange(BATCH, dtype=jnp.int32)
    query_blocks = query_wide.reshape(BATCH // height, height, D)
    target_blocks = positives.astype(jnp.int32).reshape(BATCH // height, height)

    def advance(running, inputs):
        block_queries, block_targets = inputs
        scores = jnp.dot(block_queries, passage_wide.T, preferred_element_type=jnp.float32) * logit_scale
        highest = jnp.max(scores, axis=1)
        log_norm = highest + jnp.log(jnp.sum(jnp.exp(scores - highest[:, None]), axis=1))
        onehot = (column_ids[None, :] == block_targets[:, None]).astype(jnp.float32)
        positive_score = jnp.sum(onehot * scores, axis=1)
        weights = widen((jnp.exp(scores - log_norm[:, None]) - onehot) * logit_scale)
        block_grads = jnp.dot(weights, passage_wide, preferred_element_type=jnp.float32)
        running = running + jnp.dot(weights.T, block_queries, preferred_element_type=jnp.float32)
        return running, (log_norm - positive_score, block_grads)

    passage_grads, (losses, query_grads) = lax.scan(
        advance, jnp.zeros((BATCH, D), jnp.float32), (query_blocks, target_blocks))
    return losses.reshape(BATCH), query_grads.reshape(BATCH, D), passage_grads
```

```python
import functools

import jax
import jax.numpy as jnp
from jax import lax
from jax.experimental import pallas as pl
from jax.experimental.pallas import tpu as pltpu
from jax.sharding import Mesh
from jax.sharding import PartitionSpec as P

AXES = ("x", "zl", "y", "c", "zh")
RING = 4
logit_scale = 20.0
MESSAGES = 160


class Links:
    def __init__(self, send_sem, recv_sem, zl_size, z_size):
        self.send_sem, self.recv_sem = send_sem, recv_sem
        self.count = 0
        self.open = []
        self.x, self.y, self.c = (lax.axis_index(a) for a in ("x", "y", "c"))
        self.zl_size, self.z_size = zl_size, z_size
        self.z = lax.axis_index("zh") * zl_size + lax.axis_index("zl")

    def at(self, axis, offset):
        size = {"x": RING, "y": RING, "z": self.z_size, "c": 2}[axis]
        return lax.rem(getattr(self, axis) + (offset % size), size)

    def device(self, axis, offset):
        place = self.at(axis, offset)
        if axis == "z":
            return {"zl": lax.rem(place, self.zl_size), "zh": lax.div(place, self.zl_size)}
        return {axis: place}

    def send(self, src, dst, axis, offset):
        k = self.count
        self.count += 1
        copy = pltpu.make_async_remote_copy(
            src_ref=src,
            dst_ref=dst,
            send_sem=self.send_sem.at[k],
            recv_sem=self.recv_sem.at[k],
            device_id=self.device(axis, offset),
            device_id_type=pl.DeviceIdType.MESH,
        )
        copy.start()
        self.open.append(copy)
        return copy

    def finish(self):
        for copy in self.open:
            copy.wait_send()


def gather_plane(net, qb, first, second, rows):
    def block(a, b, part=rows):
        place = {first: net.at(first, a), second: net.at(second, b)}
        return qb.at[place["x"], place["y"], part]

    def push(ref, axis, offset):
        return net.send(ref, ref, axis, offset)

    start, length = rows.start, rows.size
    top = pl.ds(start, length // 2)
    low = pl.ds(start + length // 2, length // 2)
    own = block(0, 0)
    near = [push(own, first, s) for s in (1, -1)]
    yield
    wide = {0: [push(own, second, s) for s in (1, -1)]}
    yield
    far = []
    near[0].wait_recv()
    far.append(push(block(-1, 0, top), first, 1))
    wide[-1] = [push(block(-1, 0), second, s) for s in (1, -1)]
    near[1].wait_recv()
    far.append(push(block(1, 0, low), first, -1))
    wide[1] = [push(block(1, 0), second, s) for s in (1, -1)]
    yield
    for copy in wide[0]:
        copy.wait_recv()
    last = [push(block(0, -1), second, 1)]
    yield
    for copy in far:
        copy.wait_recv()
    wide[2] = [push(block(2, 0), second, s) for s in (1, -1)]
    yield
    for copy in wide[-1]:
        copy.wait_recv()
    last.append(push(block(-1, -1), second, 1))
    for copy in wide[1]:
        copy.wait_recv()
    last.append(push(block(1, 1), second, -1))
    yield
    for copy in wide[2]:
        copy.wait_recv()
    last.append(push(block(2, 1), second, -1))
    yield
    for copy in last:
        copy.wait_recv()
    yield


def gather_line(net, pb, rows):
    half = rows // 2
    parts = (pl.ds(0, half), pl.ds(half, half))
    reach = net.z_size // 2
    across = []

    def hand_over(offset, part):
        across.append(
            net.send(
                pb.at[0, net.at("z", offset), part], pb.at[1, net.at("z", offset), part], "c", 1
            )
        )

    def push(offset, part, direction):
        ref = pb.at[0, net.at("z", offset), part]
        return net.send(ref, ref, "z", direction)

    flights = {(d, h): push(0, parts[h], d) for h in (0, 1) for d in (1, -1)}
    for part in parts:
        hand_over(0, part)
    yield
    for step in range(1, reach + 1):
        ahead = {}
        for h in (0, 1):
            for d in (1, -1):
                carried = 0 if d == 1 else 1
                if step == reach and h != carried:
                    continue
                flights[d, h].wait_recv()
                if step < reach - 1 or (step == reach - 1 and h == carried):
                    ahead[d, h] = push(-d * step, parts[h], d)
                hand_over(-d * step, parts[h])
        flights = ahead
        yield
    for copy in across:
        copy.wait_recv()
    yield


def exchange(net, axis, src, slots):
    copies = [net.send(src, slots.at[k - 1], axis, k) for k in (1, 2, 3)]
    for copy in copies:
        copy.wait_recv()


def scatter_plane(net, total, landing, late, first, second):
    def block(a, b, part=slice(None)):
        place = {first: net.at(first, a), second: net.at(second, b)}
        return total.at[place["x"], place["y"], part]

    front, back = (1, 0), (2, 3)
    far = {}
    for a, b in zip(front, back):
        far[1, a] = net.send(block(2, a), landing.at[0, a], first, 1)
        far[-1, b] = net.send(block(2, b), landing.at[1, b], first, -1)
    yield
    near = {}
    for a, b in zip(front, back):
        near[1, b] = net.send(block(1, b), landing.at[2, b], first, 1)
        near[-1, a] = net.send(block(-1, a), landing.at[3, a], first, -1)
    yield
    for a, b in zip(front, back):
        for d, k, lane in ((1, a, 0), (-1, b, 1)):
            far[d, k].wait_recv()
            ref = block(d, k)
            ref[...] += landing[lane, k]
            near[d, k] = net.send(ref, landing.at[2 + lane, k], first, d)
    yield
    half = total.shape[2] // 2
    top, low = pl.ds(0, half), pl.ds(half, half)
    hops = {}
    for k in (2, 1, 3, 0):
        near[1, k].wait_recv()
        near[-1, k].wait_recv()
        ref = block(0, k)
        ref[...] += landing[2, k] + landing[3, k]
        if k == 2:
            hops[1, 0] = net.send(block(0, 2, top), late.at[0, top], second, 1)
            hops[-1, 0] = net.send(block(0, 2, low), late.at[0, low], second, -1)
        if k == 1:
            hops[1, 1] = net.send(block(0, 1, low), late.at[1, low], second, 1)
        if k == 3:
            hops[-1, 1] = net.send(block(0, -1, top), late.at[2, top], second, -1)
    yield
    for d, part, slot in ((1, top, 1), (-1, low, 2)):
        hops[d, 0].wait_recv()
        ref = block(0, d, part)
        ref[...] += late[0, part]
        hops[d, 2] = net.send(ref, late.at[slot, part], second, d)
    yield
    for d in (1, -1):
        hops[d, 1].wait_recv()
        hops[d, 2].wait_recv()
    ref = block(0, 0)
    ref[...] += late[1] + late[2]
    yield


def scatter_line(net, total, across, landing, rows):
    reach = net.z_size // 2
    half = rows // 2
    parts = (pl.ds(0, half), pl.ds(half, half))
    order = [reach]
    for k in range(reach - 1, 0, -1):
        order += [k, -k]
    order.append(0)
    gifts = {}
    for k in order:
        place = net.at("z", k)
        gifts[k] = net.send(total.at[1, place], across.at[place], "c", 1)
    yield

    def settle(k):
        gifts[k].wait_recv()
        place = net.at("z", k)
        total[0, place] += across[place]

    flights = {}

    def push(d, h, step):
        flights[d, h] = net.send(
            total.at[0, net.at("z", d * (reach - step)), parts[h]],
            landing.at[0 if d == 1 else 1, step, parts[h]],
            "z",
            d,
        )

    settle(reach)
    push(1, 0, 0)
    push(-1, 1, 0)
    settle(reach - 1)
    push(1, 1, 1)
    settle(1 - reach)
    push(-1, 0, 1)
    yield
    for step in range(1, reach):
        if step > 1:
            settle(reach - step)
            settle(step - reach)
        for h in (0, 1):
            for d in (1, -1):
                full = (d == 1) == (h == 0)
                if not full and step == 1:
                    continue
                flights[d, h].wait_recv()
                total[0, net.at("z", d * (reach - step)), parts[h]] += landing[
                    0 if d == 1 else 1, step - 1, parts[h]
                ]
                push(d, h, step)
        yield
    settle(0)
    for copy in flights.values():
        copy.wait_recv()
    yield


def interleave(*rounds):
    rounds = list(rounds)
    while rounds:
        for r in list(rounds):
            try:
                next(r)
            except StopIteration:
                rounds.remove(r)


def kernel(
    zl_size,
    z_size,
    q_in,
    p_in,
    t_in,
    loss_out,
    qg_out,
    pg_out,
    qb,
    pb,
    tb,
    scores,
    weights,
    stats,
    stats_x,
    mid,
    stats_y,
    qga,
    qgb,
    pg,
    land_a,
    land_b,
    late_a,
    late_b,
    across,
    land_z,
    send_sem,
    recv_sem,
):
    rows, width = q_in.shape
    net = Links(send_sem, recv_sem, zl_size, z_size)
    peers = [("x", k) for k in (1, 2, 3)] + [("y", k) for k in (1, 2, 3)]
    peers += [("z", k) for k in sorted({1, z_size - 1})] + [("c", 1)]
    barrier = pltpu.get_barrier_semaphore()
    for axis, k in peers:
        pl.semaphore_signal(
            barrier,
            inc=1,
            device_id=net.device(axis, k),
            device_id_type=pl.DeviceIdType.MESH,
        )
    qb[net.x, net.y] = q_in[...].astype(jnp.bfloat16)
    pb[0, net.z] = p_in[...].astype(jnp.bfloat16)
    mine = t_in[...]
    tb[net.x, net.y] = jnp.broadcast_to(jnp.concatenate([mine] * (128 // rows), axis=1), (8, 128))
    pl.semaphore_wait(barrier, len(peers))

    half = rows // 2
    interleave(
        gather_plane(net, qb, "x", "y", pl.ds(0, half)),
        gather_plane(net, qb, "y", "x", pl.ds(half, half)),
        gather_line(net, pb, rows),
    )
    tile = tb.at[net.x, net.y]
    copies = [net.send(tile, tile, "x", k) for k in (1, 2, 3)]
    for copy in copies:
        copy.wait_recv()
    column = tb.at[:, net.y]
    copies = [net.send(column, column, "y", k) for k in (1, 2, 3)]
    for copy in copies:
        copy.wait_recv()

    group = RING * rows
    columns = 2 * z_size * rows
    band = 128
    bands = columns // band

    def target_of(xs):
        value = jnp.concatenate([tb[xs, ys, 0:1, 0:rows] for ys in range(RING)], axis=1)
        inside = lax.rem(value, rows)
        value = lax.div(value, rows)
        zh_size = z_size // zl_size
        zh = lax.rem(value, zh_size)
        value = lax.div(value, zh_size)
        core = lax.rem(value, 2)
        value = lax.div(value, 2)
        y = lax.rem(value, RING)
        value = lax.div(value, RING)
        zl = lax.rem(value, zl_size)
        x = lax.div(value, zl_size)
        local = (lax.rem(core + net.c, 2) * z_size + zh * zl_size + zl) * rows + inside
        return jnp.where((x == net.x) & (y == net.y), local, -1)

    all_passages = pb[...].reshape(columns, width)
    for xs in range(RING):
        queries = qb[xs].reshape(group, width)
        scores[xs] = (
            lax.dot_general(
                all_passages, queries, (((1,), (1,)), ((), ())), preferred_element_type=jnp.float32
            )
            * logit_scale
        )
    fold = lambda value, how: how(value.reshape(band // 8, 8, group), axis=0)
    for xs in range(RING):
        target = target_of(xs)

        def top(b, highest):
            return jnp.maximum(highest, fold(scores[xs, pl.ds(b * band, band)], jnp.max))

        highest = lax.fori_loop(0, bands, top, jnp.full((8, group), -jnp.inf, jnp.float32))
        highest = jnp.max(highest, axis=0, keepdims=True)

        def terms(b, totals):
            piece = pl.ds(b * band, band)
            value = scores[xs, piece]
            place = lax.broadcasted_iota(jnp.int32, (band, group), 0) + b * band
            hit = jnp.where(place == target, value, 0.0)
            value = jnp.exp(value - highest)
            scores[xs, piece] = value
            return totals[0] + fold(value, jnp.sum), totals[1] + fold(hit, jnp.sum)

        zero = jnp.zeros((8, group), jnp.float32)
        total, hit = lax.fori_loop(0, bands, terms, (zero, zero))
        stats[xs : xs + 1] = highest
        stats[RING + xs : RING + xs + 1] = jnp.sum(total, axis=0, keepdims=True)
        stats[2 * RING + xs : 2 * RING + xs + 1] = jnp.sum(hit, axis=0, keepdims=True)
    stats[3 * RING :] = jnp.zeros((RING, group), jnp.float32)

    def combined(own, others):
        pieces = [own[...]] + [others[k] for k in range(3)]
        tops = [piece[:RING] for piece in pieces]
        highest = functools.reduce(jnp.maximum, tops)
        total = sum(
            piece[RING : 2 * RING] * jnp.exp(top - highest) for piece, top in zip(pieces, tops)
        )
        positive = sum(piece[2 * RING : 3 * RING] for piece in pieces)
        return highest, total, positive

    exchange(net, "x", stats, stats_x)
    highest, total, positive = combined(stats, stats_x)
    mid[0:RING] = highest
    mid[RING : 2 * RING] = total
    mid[2 * RING : 3 * RING] = positive
    mid[3 * RING :] = jnp.zeros((RING, group), jnp.float32)
    exchange(net, "y", mid, stats_y)
    highest, total, positive = combined(mid, stats_y)
    log_norm = highest + jnp.log(total)
    losses = log_norm - positive
    line = lax.broadcasted_iota(jnp.int32, losses.shape, 0)
    losses = jnp.sum(jnp.where(line == net.x, losses, 0.0), axis=0, keepdims=True)
    picked = losses[:, :rows]
    for ys in range(1, RING):
        picked = jnp.where(net.y == ys, losses[:, ys * rows : (ys + 1) * rows], picked)
    loss_out[...] = picked
    factor = jnp.exp(stats[0:RING] - log_norm)

    for xs in range(RING):
        target = target_of(xs)
        scale = factor[xs : xs + 1]

        def weigh(b, carry):
            piece = pl.ds(pl.multiple_of(b * band, band), band)
            place = lax.broadcasted_iota(jnp.int32, (band, group), 0) + b * band
            onehot = jnp.where(place == target, 1.0, 0.0)
            weights[piece, xs * group : (xs + 1) * group] = (
                (scores[xs, piece] * scale - onehot) * logit_scale
            ).astype(jnp.bfloat16)
            return carry

        lax.fori_loop(0, bands, weigh, 0)

    all_queries = qb[...].reshape(RING * group, width)
    for core in (1, 0):
        some = weights[core * z_size * rows : (core + 1) * z_size * rows]
        pg[core] = jnp.dot(some, all_queries, preferred_element_type=jnp.float32).reshape(
            z_size, rows, width
        )
    for xs in range(RING):
        some = weights[:, xs * group : (xs + 1) * group]
        part = lax.dot_general(
            some, all_passages, (((0,), (0,)), ((), ())), preferred_element_type=jnp.float32
        )
        qga[xs] = part[:, : width // 2].reshape(RING, rows, width // 2)
        qgb[xs] = part[:, width // 2 :].reshape(RING, rows, width // 2)

    interleave(
        scatter_line(net, pg, across, land_z, rows),
        scatter_plane(net, qga, land_a, late_a, "x", "y"),
        scatter_plane(net, qgb, land_b, late_b, "y", "x"),
    )
    qg_out[:, : width // 2] = qga[net.x, net.y]
    qg_out[:, width // 2 :] = qgb[net.x, net.y]
    reach = z_size // 2
    pg_out[...] = pg[0, net.z] + (land_z[0, reach - 1] + land_z[1, reach - 1])
    net.finish()


def body(zl_size, z_size, queries, passages, positives):
    rows, width = queries.shape
    group = RING * rows
    columns = 2 * z_size * rows
    f32, bf16 = jnp.float32, jnp.bfloat16
    reach = z_size // 2
    losses, query_grads, passage_grads = pl.pallas_call(
        functools.partial(kernel, zl_size, z_size),
        out_shape=(
            jax.ShapeDtypeStruct((1, rows), f32),
            jax.ShapeDtypeStruct((rows, width), f32),
            jax.ShapeDtypeStruct((rows, width), f32),
        ),
        in_specs=[pl.BlockSpec(memory_space=pltpu.VMEM)] * 3,
        out_specs=[pl.BlockSpec(memory_space=pltpu.VMEM)] * 3,
        scratch_shapes=[
            pltpu.VMEM((RING, RING, rows, width), bf16),
            pltpu.VMEM((2, z_size, rows, width), bf16),
            pltpu.VMEM((RING, RING, 8, 128), jnp.int32),
            pltpu.VMEM((RING, columns, group), f32),
            pltpu.VMEM((columns, RING * group), bf16),
            pltpu.VMEM((4 * RING, group), f32),
            pltpu.VMEM((3, 4 * RING, group), f32),
            pltpu.VMEM((4 * RING, group), f32),
            pltpu.VMEM((3, 4 * RING, group), f32),
            pltpu.VMEM((RING, RING, rows, width // 2), f32),
            pltpu.VMEM((RING, RING, rows, width // 2), f32),
            pltpu.VMEM((2, z_size, rows, width), f32),
            pltpu.VMEM((4, RING, rows, width // 2), f32),
            pltpu.VMEM((4, RING, rows, width // 2), f32),
            pltpu.VMEM((3, rows, width // 2), f32),
            pltpu.VMEM((3, rows, width // 2), f32),
            pltpu.VMEM((z_size, rows, width), f32),
            pltpu.VMEM((2, reach, rows, width), f32),
            pltpu.SemaphoreType.DMA((MESSAGES,)),
            pltpu.SemaphoreType.DMA((MESSAGES,)),
        ],
        compiler_params=pltpu.CompilerParams(
            collective_id=0, has_side_effects=True, vmem_limit_bytes=60 * 1024 * 1024
        ),
    )(queries, passages, positives.reshape(1, rows))
    return losses.reshape(rows), query_grads, passage_grads


def solution(mesh):
    zl_size, z_hi = 2, mesh.shape["sub"]
    torus = Mesh(mesh.devices.reshape(RING, zl_size, RING, 2, z_hi), AXES)
    return jax.shard_map(
        functools.partial(body, zl_size, zl_size * z_hi),
        mesh=torus,
        in_specs=(P(AXES, None), P(AXES, None), P(AXES)),
        out_specs=(P(AXES), P(AXES, None), P(AXES, None)),
        check_vma=False,
    )
```

```python
import functools

import jax
import jax.numpy as jnp
from jax import lax
from jax.experimental import pallas as pl
from jax.experimental.pallas import tpu as pltpu
from jax.sharding import Mesh
from jax.sharding import PartitionSpec as P

AXES = ("x", "zl", "y", "c", "zh")
RING = 4
logit_scale = 20.0
SIGNALS = 136

WIRE = {"x": 0.022, "y": 0.022, "z": 0.022, "c": 0.0016}
DELAY = {"x": 2.4, "y": 2.4, "z": 2.5, "c": 1.0}


class Place:
    def __init__(self, zl_size, z_size):
        self.x, self.y, self.c = (lax.axis_index(a) for a in ("x", "y", "c"))
        self.zl_size, self.z_size = zl_size, z_size
        self.z = lax.axis_index("zh") * zl_size + lax.axis_index("zl")

    def at(self, axis, offset):
        size = {"x": RING, "y": RING, "z": self.z_size, "c": 2}[axis]
        return lax.rem(getattr(self, axis) + (offset % size), size)

    def device(self, axis, offset):
        place = self.at(axis, offset)
        if axis == "z":
            return {"zl": lax.rem(place, self.zl_size), "zh": lax.div(place, self.zl_size)}
        return {axis: place}


class Plan:
    def __init__(self, place, recv_sem, send_sems):
        self.place, self.recv_sem, self.send_sems = place, recv_sem, send_sems
        self.tasks = []
        self.slots = {}
        self.copies = {}
        self.sent = {}

    def task(self, name, needs=(), run=None, sends=(), cost=0.05, rank=0):
        self.tasks.append((name, tuple(needs), run, tuple(sends), cost, rank))

    def order(self):
        waiting = list(enumerate(self.tasks))
        known, link, now, result = {}, {}, 0.0, []
        while waiting:
            ready = []
            for index, task in waiting:
                if all(n in known for n in task[1]):
                    ready.append((max([known[n] for n in task[1]], default=0.0), task[5], index, task))
            due = [r for r in ready if r[0] <= now]
            pick = min(due, key=lambda r: (r[1], r[2])) if due else min(ready, key=lambda r: r[:3])
            start, _, index, task = pick
            now = max(now, start) + task[4]
            known[task[0]] = now
            for message, axis, offset, kib, _, _ in task[3]:
                lane = (axis, offset)
                link[lane] = max(link.get(lane, 0.0), now) + kib * WIRE[axis]
                known[message] = link[lane] + DELAY[axis]
            waiting = [w for w in waiting if w[0] != index]
            result.append(task)
        return result

    def signal(self, message):
        kind = message.split("_")[0]
        if kind == "rs":
            kind = "qg"
        group = self.slots.setdefault(message.split("_")[0], {})
        number = group.setdefault(message, len(group))
        base = {"qg": 0, "pg": 60, "tg": 96, "st": 102, "rz": 108}[kind]
        return self.recv_sem.at[base + number]

    def run(self):
        got = set()
        for name, needs, run, sends, _, _ in self.order():
            for need in needs:
                if need in self.copies and need not in got:
                    got.add(need)
                    self.copies[need].wait_recv()
            if run is not None:
                run()
            for message, axis, offset, kib, pool, refs in sends:
                src, dst = refs()
                copy = pltpu.make_async_remote_copy(
                    src_ref=src,
                    dst_ref=dst,
                    send_sem=self.send_sems.at[pool],
                    recv_sem=self.signal(message),
                    device_id=self.place.device(axis, offset),
                    device_id_type=pl.DeviceIdType.MESH,
                )
                copy.start()
                self.copies[message] = copy
                self.sent[pool] = self.sent.get(pool, 0) + kib
        missed = set(self.copies) - got
        assert not missed, missed

    def finish(self, ref, pool, per_kib=1):
        dummy = ref.at[pl.ds(0, self.sent[pool] // per_kib)]
        pltpu.make_async_remote_copy(
            src_ref=dummy,
            dst_ref=dummy,
            send_sem=self.send_sems.at[pool],
            recv_sem=self.recv_sem.at[0],
            device_id=self.place.device("c", 1),
            device_id_type=pl.DeviceIdType.MESH,
        ).wait_send()


def slot_of(offset, z_size):
    offset = offset % z_size
    if offset == 0:
        return 0
    if offset <= z_size // 2:
        return 2 * offset - 1
    return 2 * (z_size - offset)


def plan_query_gather(plan, qb, first, second, pieces, quarter):
    place = plan.place
    kib = 32
    brings = {}

    def ref(a, b, p):
        at = {first: place.at(first, a), second: place.at(second, b)}
        return qb.at[at["x"], at["y"], pl.ds(p * quarter, quarter)]

    def send(kind, a, b, p, axis, d):
        name = f"qg_{first}{kind}{a}{p}{d}"
        to = (a - d, b) if axis == first else (a, b - d)
        key = ((to[0] + 1) % 4 - 1, (to[1] + 1) % 4 - 1)
        brings.setdefault(key, []).append(name)
        both = lambda: (ref(a, b, p),) * 2
        return name, (name, axis, d, kib, 0, both)

    u, v = pieces
    opening, names = [], {}
    for p in pieces:
        for d in (1, -1):
            names["f", p, d], s = send("f", 0, 0, p, first, d)
            opening.append((s, p, d))
    opening.sort(key=lambda o: (o[1] == u) != (o[2] == 1))
    start = [o[0] for o in opening]

    def wide(a, p):
        result = []
        for d in (1, -1):
            names["w", a, p, d], s = send("w", a, 0, p, second, d)
            result.append(s)
        return result

    widest = [s for p in pieces for s in wide(0, p)]
    names["far", u], far_u = send("g", -1, 0, u, first, 1)
    plan.task(f"{first}f-1{u}", [names["f", u, 1]], sends=[far_u] + wide(-1, u))
    names["far", v], far_v = send("g", 1, 0, v, first, -1)
    plan.task(f"{first}f1{v}", [names["f", v, -1]], sends=[far_v] + wide(1, v))
    plan.task(f"{first}f-1{v}", [names["f", v, 1]], sends=wide(-1, v))
    plan.task(f"{first}f1{u}", [names["f", u, -1]], sends=wide(1, u))
    for p in pieces:
        plan.task(f"{first}g{p}", [names["far", p]], sends=wide(2, p))
    for a in (0, -1, 1, 2):
        for p, b, d in ((u, -1, 1), (v, 1, -1)):
            _, s = send("l", a, b, p, second, d)
            plan.task(f"{first}l{a}{p}", [names["w", a, p, d]], sends=[s])
    return start, widest, brings


def plan_passage_gather(plan, pb, quarter):
    z_size = plan.place.z_size
    reach = z_size // 2
    carried = {1: (0, 1), -1: (2, 3)}
    names = []
    start = []

    def ref(offset, p):
        return pb.at[slot_of(offset, z_size), 0, pl.ds(p * quarter, quarter)]

    def push(step, p, d):
        both = lambda: (ref(-d * step, p), ref(-d * (step + 1), p))
        return (f"pg_{step + 1}{p}{d}", "z", d, 32, 0, both)

    def hand_over(offset):
        s = slot_of(offset, z_size)
        names.append(f"pg_c{s}")
        return (f"pg_c{s}", "c", 1, 128, 0, lambda: (pb.at[s, 0], pb.at[s, 1]))

    for d in (1, -1):
        for p in carried[d] + carried[-d]:
            start.append(push(0, p, d))
    for step in range(1, reach):
        for d in (1, -1):
            for p in carried[d] + carried[-d]:
                sends = []
                if step < reach - 1 or p in carried[d]:
                    sends.append(push(step, p, d))
                plan.task(f"z{step}{p}{d}", [f"pg_{step}{p}{d}"], sends=sends)
            plan.task(
                f"h{step}{d}",
                [f"pg_{step}{p}{d}" for p in range(4)],
                sends=[hand_over(-d * step)],
            )
    plan.task(
        f"h{reach}",
        [f"pg_{reach}{p}{d}" for d in (1, -1) for p in carried[d]],
        sends=[hand_over(reach)],
    )
    start.append(hand_over(0))
    return start, names


def plan_plane_scatter(plan, total, landing, late, first, second, ready):
    place = plan.place
    half = total.shape[2] // 2
    parts = (pl.ds(0, half), pl.ds(half, half))
    kib = 64

    def ref(a, b, h=None):
        at = {first: place.at(first, a), second: place.at(second, b)}
        if h is None:
            return total.at[at["x"], at["y"]]
        return total.at[at["x"], at["y"], parts[h]]

    def send(kind, a, b, h, axis, d, dst):
        name = f"rs_{first}{kind}{b}{h}{d}"
        return (name, axis, d, kib, 1, lambda: (ref(a, b, h), dst()))

    def far(k):
        return [
            send("f", 2, k, h, first, d, lambda h=h: landing.at[0, k % RING, parts[h]])
            for h, d in ((0, 1), (1, -1))
        ]

    def own(k):
        return [
            send("n", d, k, h, first, d, lambda h=h, d=d: landing.at[1 if d == 1 else 2, k % RING, parts[h]])
            for h, d in ((1, 1), (0, -1))
        ]

    def acc(k, more, needs=()):
        def run():
            for h, d in ((0, 1), (1, -1)):
                ref(d, k, h)[...] += landing[0, k % RING, parts[h]]

        sends = [
            send("n", d, k, h, first, d, lambda h=h, d=d: landing.at[1 if d == 1 else 2, k % RING, parts[h]])
            for h, d in ((0, 1), (1, -1))
        ]
        needs = [f"rs_{first}f{k}{h}{d}" for h, d in ((0, 1), (1, -1))] + list(needs)
        plan.task(f"{first}acc{k}", needs, run, sends + more, cost=0.15)

    plan.task(f"{first}far2", [ready(2, 2)], sends=far(2))
    plan.task(f"{first}own2", [ready(1, 2), ready(-1, 2)], sends=own(2))
    plan.task(f"{first}far1", [ready(2, 1)], sends=far(1))
    everything = [ready(a, b) for a in (0, 1, 2, -1) for b in (0, 1, 2, -1)]
    acc(2, own(1) + far(-1), everything)
    acc(1, own(-1) + far(0))
    acc(-1, own(0))
    acc(0, [])

    def done(k, sends):
        def run():
            ref(0, k)[...] += landing[1, k % RING] + landing[2, k % RING]

        needs = [f"rs_{first}n{k}{h}{d}" for h in (0, 1) for d in (1, -1)]
        plan.task(f"{first}done{k}", needs, run, sends, cost=0.1)

    def hop(kind, b, h, d, slot):
        return send(kind, 0, b, h, second, d, lambda: late.at[slot, parts[h]])

    done(2, [hop("s", 2, 0, 1, 0), hop("s", 2, 1, -1, 0)])
    done(1, [hop("s", 1, 1, 1, 1)])
    done(-1, [hop("s", -1, 0, -1, 2)])
    done(0, [])
    for d, h, slot in ((1, 0, 1), (-1, 1, 2)):

        def run(d=d, h=h):
            ref(0, d, h)[...] += late[0, parts[h]]

        plan.task(
            f"{first}turn{d}",
            [f"rs_{first}s2{h}{d}", f"{first}done{d}"],
            run,
            [hop("t", d, h, d, slot)],
            cost=0.1,
        )
    last = [f"rs_{first}s11{1}", f"rs_{first}s-10{-1}", f"rs_{first}t10{1}", f"rs_{first}t-11{-1}"]
    return last + [f"{first}done0"]


def plan_line_scatter(plan, total, across, landing, rows, ready):
    z_size = plan.place.z_size
    reach = z_size // 2
    half = rows // 2
    parts = (pl.ds(0, half), pl.ds(half, half))

    def settle(k):
        s = slot_of(k, z_size)
        total[s, 0] += across[s]

    def push(d, h, step):
        s = slot_of(d * (reach - step), z_size)
        both = lambda: (total.at[s, 0, parts[h]], landing.at[0 if d == 1 else 1, step, parts[h]])
        return (f"rz_{d}{h}{step}", "z", d, 128, 2, both)

    for k in [reach] + [s for k in range(reach - 1, 0, -1) for s in (k, -k)] + [0]:
        s = slot_of(k, z_size)
        gift = (f"rz_c{s}", "c", 1, 256, 2, lambda s=s: (total.at[s, 1], across.at[s]))
        plan.task(f"gift{s}", [ready(s)], sends=[gift])
        sends = []
        if k == reach:
            sends = [push(1, 0, 0), push(-1, 1, 0)]
        elif k == reach - 1:
            sends = [push(1, 1, 1)]
        elif k == 1 - reach:
            sends = [push(-1, 0, 1)]
        plan.task(f"settle{s}", [f"rz_c{s}", f"gift{s}"], lambda k=k: settle(k), sends, cost=0.12)
    for step in range(1, reach):
        for d in (1, -1):
            for h in (0, 1):
                full = (d == 1) == (h == 0)
                if not full and step == 1:
                    continue
                s = slot_of(d * (reach - step), z_size)

                def run(d=d, h=h, s=s, step=step):
                    total[s, 0, parts[h]] += landing[0 if d == 1 else 1, step - 1, parts[h]]

                plan.task(
                    f"rz{d}{h}{step}",
                    [f"rz_{d}{h}{step - 1}", f"settle{s}"],
                    run,
                    [push(d, h, step)],
                    cost=0.1,
                )
    return [f"rz_{d}{h}{reach - 1}" for d in (1, -1) for h in (0, 1)] + ["settle0"]


def kernel(
    zl_size,
    z_size,
    q_in,
    p_in,
    t_in,
    loss_out,
    qg_out,
    pg_out,
    qb,
    pb,
    tb,
    scores,
    weights,
    stats,
    stats_x,
    mid,
    stats_y,
    factor,
    qga,
    qgb,
    pg,
    land_a,
    land_b,
    late_a,
    late_b,
    across,
    land_z,
    send_sem,
    recv_sem,
):
    rows, width = q_in.shape
    quarter = rows // 4
    group = RING * rows
    columns = 2 * z_size * rows
    place = Place(zl_size, z_size)
    peers = [("x", k) for k in (1, 2, 3)] + [("y", k) for k in (1, 2, 3)]
    peers += [("z", 1), ("z", z_size - 1), ("c", 1)]
    barrier = pltpu.get_barrier_semaphore()
    for axis, k in peers:
        pl.semaphore_signal(
            barrier,
            inc=1,
            device_id=place.device(axis, k),
            device_id_type=pl.DeviceIdType.MESH,
        )
    qb[place.x, place.y] = q_in[...].astype(jnp.bfloat16)
    pb[0, 0] = p_in[...].astype(jnp.bfloat16)
    mine = t_in[...]
    tb[place.x * RING + place.y] = jnp.broadcast_to(
        jnp.concatenate([mine] * (128 // rows), axis=1), (8, 128)
    )
    pl.semaphore_wait(barrier, len(peers))

    plan = Plan(place, recv_sem, send_sem)

    start_a, wide_a, brings_a = plan_query_gather(plan, qb, "x", "y", (0, 1), quarter)
    start_b, wide_b, brings_b = plan_query_gather(plan, qb, "y", "x", (2, 3), quarter)
    start_p, crossing = plan_passage_gather(plan, pb, quarter)

    def tile():
        return (tb.at[place.x * RING + place.y],) * 2

    def tiles():
        return (tb.at[pl.ds(place.x * RING, RING)],) * 2

    ty = [(f"tg_y{k}", "y", k, 4, 3, tile) for k in (1, 2, 3)]
    tx = [(f"tg_x{k}", "x", k, 16, 3, tiles) for k in (1, 2, 3)]
    plan.task("open", sends=start_p + start_a + start_b + ty + wide_a + wide_b, rank=-1)
    plan.task("ty", [s[0] for s in ty], sends=tx)

    def at_x(a):
        return place.at("x", a)

    def spot(a):
        return pl.ds(pl.multiple_of(at_x(a) * columns, columns), columns)

    def multiply(a, h):
        size = columns // 2
        some = pb[h * z_size // 2 : (h + 1) * z_size // 2].reshape(size, width)
        queries = qb[at_x(a)].reshape(group, width)
        start = pl.multiple_of(at_x(a) * columns + h * size, size)
        scores[pl.ds(start, size)] = (
            lax.dot_general(
                some, queries, (((1,), (1,)), ((), ())), preferred_element_type=jnp.float32
            )
            * logit_scale
        )

    band = 128
    bands = columns // band

    def target_of(a):
        line = at_x(a) * RING
        value = jnp.concatenate([tb[line + ys, 0:1, 0:rows] for ys in range(RING)], axis=1)
        inside = lax.rem(value, rows)
        value = lax.div(value, rows)
        zh_size = z_size // zl_size
        zh = lax.rem(value, zh_size)
        value = lax.div(value, zh_size)
        core = lax.rem(value, 2)
        value = lax.div(value, 2)
        y = lax.rem(value, RING)
        value = lax.div(value, RING)
        zl = lax.rem(value, zl_size)
        x = lax.div(value, zl_size)
        apart = lax.rem(zh * zl_size + zl - place.z + z_size, z_size)
        slot = jnp.where(apart == 0, 0, jnp.where(apart <= z_size // 2, 2 * apart - 1, 2 * (z_size - apart)))
        local = (slot * 2 + lax.rem(core + place.c, 2)) * rows + inside
        return jnp.where((x == place.x) & (y == place.y), local, -1)

    def fold(value, how):
        return how(value.reshape(band // 8, 8, group), axis=0)

    def piece_of(a, b):
        return pl.ds(pl.multiple_of(at_x(a) * columns + b * band, band), band)

    def measure(a):
        target = target_of(a)

        def top(b, highest):
            return jnp.maximum(highest, fold(scores[piece_of(a, b)], jnp.max))

        highest = lax.fori_loop(0, bands, top, jnp.full((8, group), -jnp.inf, jnp.float32))
        highest = jnp.max(highest, axis=0, keepdims=True)

        def terms(b, totals):
            value = scores[piece_of(a, b)]
            spots = lax.broadcasted_iota(jnp.int32, (band, group), 0) + b * band
            hit = jnp.where(spots == target, value, 0.0)
            value = jnp.exp(value - highest)
            scores[piece_of(a, b)] = value
            return totals[0] + fold(value, jnp.sum), totals[1] + fold(hit, jnp.sum)

        zero = jnp.zeros((8, group), jnp.float32)
        total, hit = lax.fori_loop(0, bands, terms, (zero, zero))
        for k, value in enumerate(
            (highest, jnp.sum(total, axis=0, keepdims=True), jnp.sum(hit, axis=0, keepdims=True))
        ):
            stats[pl.ds(k * RING + at_x(a), 1)] = value

    near_half = [f"pg_c{s}" for s in range(z_size // 2)]
    for s in range(1, z_size // 2):
        k = (s + 1) // 2 * (1 if s % 2 else -1)
        near_half.append(f"h{abs(k)}{-1 if k > 0 else 1}")
    whole = [t[0] for t in plan.tasks if t[0].startswith("h")]
    for rank, a in enumerate((0, -1, 1, 2)):
        needs = [n for b in (-1, 0, 1, 2) for n in brings_a.get((a, b), []) + brings_b.get((b, a), [])]
        plan.task(f"mul{a}0", needs + near_half, lambda a=a: multiply(a, 0), cost=0.45, rank=1 + rank)
        plan.task(
            f"mul{a}1",
            [f"mul{a}0"] + whole + crossing,
            lambda a=a: multiply(a, 1),
            cost=0.45,
            rank=1 + rank,
        )
        plan.task(
            f"measure{a}",
            [f"mul{a}1"] + [s[0] for s in tx],
            lambda a=a: measure(a),
            cost=0.5,
            rank=1 + rank,
        )

    def combined(own, others):
        pieces = [own[...]] + [others[k] for k in range(3)]
        tops = [piece[:RING] for piece in pieces]
        highest = functools.reduce(jnp.maximum, tops)
        total = sum(
            piece[RING : 2 * RING] * jnp.exp(top - highest) for piece, top in zip(pieces, tops)
        )
        positive = sum(piece[2 * RING : 3 * RING] for piece in pieces)
        return highest, total, positive

    def half_way():
        highest, total, positive = combined(stats, stats_x)
        mid[0:RING] = highest
        mid[RING : 2 * RING] = total
        mid[2 * RING : 3 * RING] = positive

    def normalise():
        highest, total, positive = combined(mid, stats_y)
        log_norm = highest + jnp.log(total)
        losses = log_norm - positive
        line = lax.broadcasted_iota(jnp.int32, losses.shape, 0)
        losses = jnp.sum(jnp.where(line == place.x, losses, 0.0), axis=0, keepdims=True)
        picked = losses[:, :rows]
        for ys in range(1, RING):
            picked = jnp.where(place.y == ys, losses[:, ys * rows : (ys + 1) * rows], picked)
        loss_out[...] = picked
        factor[0:RING] = jnp.exp(stats[0:RING] - log_norm)

    def blank():
        stats[3 * RING :] = jnp.zeros((RING, group), jnp.float32)
        mid[3 * RING :] = jnp.zeros((RING, group), jnp.float32)
        factor[RING:] = jnp.zeros((RING, group), jnp.float32)

    plan.task("blank", run=blank)
    sx = [(f"st_x{k}", "x", k, 16, 0, lambda k=k: (stats, stats_x.at[k - 1])) for k in (1, 2, 3)]
    sy = [(f"st_y{k}", "y", k, 16, 0, lambda k=k: (mid, stats_y.at[k - 1])) for k in (1, 2, 3)]
    everything = [t[0] for t in plan.tasks]
    plan.task("sx", everything, sends=sx)
    plan.task("half", [s[0] for s in sx], half_way, sy)
    plan.task("norm", [s[0] for s in sy], normalise)

    def weigh(a):
        target = target_of(a)
        scale = factor[pl.ds(at_x(a), 1)]
        lanes = pl.ds(pl.multiple_of(at_x(a) * group, group), group)

        def step(b, carry):
            spots = lax.broadcasted_iota(jnp.int32, (band, group), 0) + b * band
            onehot = jnp.where(spots == target, 1.0, 0.0)
            weights[pl.ds(pl.multiple_of(b * band, band), band), lanes] = (
                (scores[piece_of(a, b)] * scale - onehot) * logit_scale
            ).astype(jnp.bfloat16)
            return carry

        lax.fori_loop(0, bands, step, 0)

    def passage_terms(first, last):
        some = weights[first * 2 * rows : last * 2 * rows]
        queries = qb[...].reshape(RING * group, width)
        pg[first:last] = jnp.dot(some, queries, preferred_element_type=jnp.float32).reshape(
            last - first, 2, rows, width
        )

    def query_terms(a):
        some = weights[:, pl.ds(pl.multiple_of(at_x(a) * group, group), group)]
        part = lax.dot_general(
            some,
            pb[...].reshape(columns, width),
            (((0,), (0,)), ((), ())),
            preferred_element_type=jnp.float32,
        )
        qga[at_x(a)] = part[:, : width // 2].reshape(RING, rows, width // 2)
        qgb[at_x(a)] = part[:, width // 2 :].reshape(RING, rows, width // 2)

    def all_weights():
        for a in (2, 1, -1, 0):
            weigh(a)

    cut = z_size - 3
    plan.task("weights", ["norm"], all_weights, cost=0.5)
    plan.task("pterms0", ["weights"], lambda: passage_terms(cut, z_size), cost=0.8)
    plan.task("qterms2", ["pterms0"], lambda: query_terms(2), cost=0.8, rank=1)
    plan.task("qterms1", ["qterms2"], lambda: query_terms(1), cost=0.8, rank=2)
    plan.task("qterms-1", ["qterms1"], lambda: query_terms(-1), cost=0.8, rank=2)
    plan.task("pterms1", ["qterms-1"], lambda: passage_terms(0, cut), cost=1.2, rank=3)
    plan.task("qterms0", ["pterms1"], lambda: query_terms(0), cost=0.8, rank=4)

    def chunk(a):
        return f"qterms{(a + 1) % 4 - 1}"

    end_a = plan_plane_scatter(plan, qga, land_a, late_a, "x", "y", lambda a, b: chunk(a))
    end_b = plan_plane_scatter(plan, qgb, land_b, late_b, "y", "x", lambda a, b: chunk(b))
    end_p = plan_line_scatter(
        plan, pg, across, land_z, rows, lambda s: "pterms0" if s >= cut else "pterms1"
    )

    def out_a():
        qg_out[:, : width // 2] = qga[place.x, place.y] + late_a[1] + late_a[2]

    def out_b():
        qg_out[:, width // 2 :] = qgb[place.x, place.y] + late_b[1] + late_b[2]

    def out_p():
        last = z_size // 2 - 1
        pg_out[...] = pg[0, 0] + (land_z[0, last] + land_z[1, last])

    plan.task("out_a", end_a, out_a)
    plan.task("out_b", end_b, out_b)
    plan.task("out_p", end_p, out_p)
    plan.run()
    plan.finish(scores, 0)
    plan.finish(scores, 1)
    plan.finish(scores, 2)
    plan.finish(tb, 3, per_kib=4)


def put_out(*refs):
    for source, target in zip(refs[:3], refs[3:]):
        target[...] = source[...]


def body(zl_size, z_size, queries, passages, positives):
    rows, width = queries.shape
    group = RING * rows
    columns = 2 * z_size * rows
    f32, bf16 = jnp.float32, jnp.bfloat16
    reach = z_size // 2
    shapes = (
        jax.ShapeDtypeStruct((1, rows), f32),
        jax.ShapeDtypeStruct((rows, width), f32),
        jax.ShapeDtypeStruct((rows, width), f32),
    )
    landing = pltpu.VMEM((3, RING, rows, width // 2), f32)
    results = pl.pallas_call(
        functools.partial(kernel, zl_size, z_size),
        out_shape=shapes,
        in_specs=[pl.BlockSpec(memory_space=pltpu.VMEM)] * 3,
        out_specs=[pl.BlockSpec(memory_space=pltpu.VMEM)] * 3,
        scratch_shapes=[
            pltpu.VMEM((RING, RING, rows, width), bf16),
            pltpu.VMEM((z_size, 2, rows, width), bf16),
            pltpu.VMEM((RING * RING, 8, 128), jnp.int32),
            pltpu.VMEM((RING * columns, group), f32),
            pltpu.VMEM((columns, RING * group), bf16),
            pltpu.VMEM((4 * RING, group), f32),
            pltpu.VMEM((3, 4 * RING, group), f32),
            pltpu.VMEM((4 * RING, group), f32),
            pltpu.VMEM((3, 4 * RING, group), f32),
            pltpu.VMEM((2 * RING, group), f32),
            pltpu.VMEM((RING, RING, rows, width // 2), f32),
            pltpu.VMEM((RING, RING, rows, width // 2), f32),
            pltpu.VMEM((z_size, 2, rows, width), f32),
            landing,
            landing,
            pltpu.VMEM((3, rows, width // 2), f32),
            pltpu.VMEM((3, rows, width // 2), f32),
            pltpu.VMEM((z_size, rows, width), f32),
            pltpu.VMEM((2, reach, rows, width), f32),
            pltpu.SemaphoreType.DMA((4,)),
            pltpu.SemaphoreType.DMA((SIGNALS,)),
        ],
        compiler_params=pltpu.CompilerParams(
            collective_id=0, has_side_effects=True, vmem_limit_bytes=56 * 1024 * 1024
        ),
    )(queries, passages, positives.reshape(1, rows))
    losses, query_grads, passage_grads = pl.pallas_call(
        put_out,
        out_shape=shapes,
        in_specs=[pl.BlockSpec(memory_space=pltpu.VMEM)] * 3,
        out_specs=[pl.BlockSpec(memory_space=pltpu.VMEM)] * 3,
    )(*results)
    return losses.reshape(rows), query_grads, passage_grads


def solution(mesh):
    zl_size, z_hi = 2, mesh.shape["sub"]
    torus = Mesh(mesh.devices.reshape(RING, zl_size, RING, 2, z_hi), AXES)
    return jax.shard_map(
        functools.partial(body, zl_size, zl_size * z_hi),
        mesh=torus,
        in_specs=(P(AXES, None), P(AXES, None), P(AXES)),
        out_specs=(P(AXES), P(AXES, None), P(AXES, None)),
        check_vma=False,
    )
```

```python
import functools

import jax
import jax.numpy as jnp
from jax import lax
from jax.experimental import pallas as pl
from jax.experimental.pallas import tpu as pltpu
from jax.sharding import Mesh
from jax.sharding import PartitionSpec as P

AXES = ("x", "zl", "y", "c", "zh")
RING = 4
logit_scale = 20.0
SIGNALS = 144

WIRE = {"x": 0.022, "y": 0.022, "z": 0.022, "c": 0.0016}
DELAY = {"x": 2.6, "y": 2.6, "z": 2.6, "c": 0.9}


class Place:
    def __init__(self, zl_size, z_size):
        self.x, self.y, self.c = (lax.axis_index(a) for a in ("x", "y", "c"))
        self.zl_size, self.z_size = zl_size, z_size
        self.z = lax.axis_index("zh") * zl_size + lax.axis_index("zl")

    def at(self, axis, offset):
        size = {"x": RING, "y": RING, "z": self.z_size, "c": 2}[axis]
        return lax.rem(getattr(self, axis) + (offset % size), size)

    def device(self, axis, offset):
        place = self.at(axis, offset)
        if axis == "z":
            return {"zl": lax.rem(place, self.zl_size), "zh": lax.div(place, self.zl_size)}
        return {axis: place}


class Plan:
    def __init__(self, place, recv_sem, send_sems):
        self.place, self.recv_sem, self.send_sems = place, recv_sem, send_sems
        self.tasks = []
        self.slots = {}
        self.copies = {}
        self.sent = {}

    def task(self, name, needs=(), run=None, sends=(), cost=0.05, rank=0):
        self.tasks.append((name, tuple(needs), run, tuple(sends), cost, rank))

    def order(self):
        waiting = list(enumerate(self.tasks))
        known, link, now, result = {}, {}, 0.0, []
        while waiting:
            ready = []
            for index, task in waiting:
                if all(n in known for n in task[1]):
                    ready.append((max([known[n] for n in task[1]], default=0.0), task[5], index, task))
            due = [r for r in ready if r[0] <= now]
            pick = min(due, key=lambda r: (r[1], r[2])) if due else min(ready, key=lambda r: r[:3])
            start, _, index, task = pick
            now = max(now, start) + task[4]
            known[task[0]] = now
            for message, axis, offset, kib, _, _ in task[3]:
                if axis in "xy" and offset == 2:
                    for lane in ((axis, 1), (axis, -1)):
                        link[lane] = max(link.get(lane, 0.0), now) + kib * WIRE[axis]
                    known[message] = max(link[axis, 1], link[axis, -1]) + DELAY[axis] + 0.6
                    continue
                far = abs(offset)
                lane = (axis, offset // far)
                link[lane] = max(link.get(lane, 0.0), now) + kib * WIRE[axis] * far
                known[message] = link[lane] + DELAY[axis] + 0.5 * (far - 1)
            waiting = [w for w in waiting if w[0] != index]
            result.append(task)
        return result

    def signal(self, message):
        kind = message.split("_")[0]
        if kind == "rs":
            kind = "qg"
        group = self.slots.setdefault(message.split("_")[0], {})
        number = group.setdefault(message, len(group))
        base = {"qg": 0, "pg": 60, "tg": 96, "st": 102, "rz": 108}[kind]
        return self.recv_sem.at[base + number]

    def run(self):
        got = set()
        for name, needs, run, sends, _, _ in self.order():
            for need in needs:
                if need in self.copies and need not in got:
                    got.add(need)
                    self.copies[need].wait_recv()
            if run is not None:
                run()
            for message, axis, offset, kib, pool, refs in sends:
                src, dst = refs()
                copy = pltpu.make_async_remote_copy(
                    src_ref=src,
                    dst_ref=dst,
                    send_sem=self.send_sems.at[pool],
                    recv_sem=self.signal(message),
                    device_id=self.place.device(axis, offset),
                    device_id_type=pl.DeviceIdType.MESH,
                )
                copy.start()
                self.copies[message] = copy
                self.sent[pool] = self.sent.get(pool, 0) + kib
        missed = set(self.copies) - got
        assert not missed, missed

    def finish(self, ref, pool, per_kib=1):
        dummy = ref.at[pl.ds(0, self.sent[pool] // per_kib)]
        pltpu.make_async_remote_copy(
            src_ref=dummy,
            dst_ref=dummy,
            send_sem=self.send_sems.at[pool],
            recv_sem=self.recv_sem.at[0],
            device_id=self.place.device("c", 1),
            device_id_type=pl.DeviceIdType.MESH,
        ).wait_send()


def unrolled(first, last, step, carry):
    for k in range(first, last):
        carry = step(k, carry)
    return carry


def slot_of(offset, z_size):
    offset = offset % z_size
    if offset == 0:
        return 0
    if offset <= z_size // 2:
        return 2 * offset - 1
    return 2 * (z_size - offset)


def plan_query_gather(plan, qb, first, second, pieces, quarter):
    place = plan.place
    kib = 32
    brings = {}

    def ref(a, b, p):
        at = {first: place.at(first, a), second: place.at(second, b)}
        return qb.at[at["x"], at["y"], pl.ds(p * quarter, quarter)]

    def send(kind, a, b, p, axis, d):
        name = f"qg_{first}{kind}{a}{p}{d}"
        to = (a - d, b) if axis == first else (a, b - d)
        key = ((to[0] + 1) % 4 - 1, (to[1] + 1) % 4 - 1)
        brings.setdefault(key, []).append(name)
        both = lambda: (ref(a, b, p),) * 2
        return name, (name, axis, d, kib, 0, both)

    u, v = pieces
    opening, names = [], {}
    for p in pieces:
        for d in (1, -1):
            names["f", p, d], s = send("f", 0, 0, p, first, d)
            opening.append((s, p, d))
    opening.sort(key=lambda o: (o[1] == u) != (o[2] == 1))
    start = [o[0] for o in opening]

    def wide(a, p):
        result = []
        for d in (1, -1):
            names["w", a, p, d], s = send("w", a, 0, p, second, d)
            result.append(s)
        return result

    widest = [s for p in pieces for s in wide(0, p)]
    for p in pieces:
        names["far", p], s = send("g", 0, 0, p, first, 2)
        widest.append(s)
    for p in pieces:
        plan.task(f"{first}f-1{p}", [names["f", p, 1]], sends=wide(-1, p))
        plan.task(f"{first}f1{p}", [names["f", p, -1]], sends=wide(1, p))
    for p in pieces:
        plan.task(f"{first}g{p}", [names["far", p]], sends=wide(2, p))
    for a in (0, -1, 1, 2):
        for p, b, d in ((u, -1, 1), (v, 1, -1)):
            _, s = send("l", a, b, p, second, d)
            plan.task(f"{first}l{a}{p}", [names["w", a, p, d]], sends=[s])
    return start, widest, brings


def plan_passage_gather(plan, pb, quarter):
    z_size = plan.place.z_size
    reach = z_size // 2
    carried = {1: (0, 1), -1: (2, 3)}
    names = []
    start = []

    def ref(offset, p):
        return pb.at[slot_of(offset, z_size), 0, pl.ds(p * quarter, quarter)]

    def push(step, p, d, places=1):
        both = lambda: (ref(-d * step, p), ref(-d * (step + places), p))
        return (f"pg_{step + places}{p}{d}", "z", d * places, 32, 0, both)

    def hand_over(offset):
        s = slot_of(offset, z_size)
        names.append(f"pg_c{s}")
        return (f"pg_c{s}", "c", 1, 128, 0, lambda: (pb.at[s, 0], pb.at[s, 1]))

    for d in (1, -1):
        for p in carried[d] + carried[-d]:
            start.append(push(0, p, d))
    for step in range(1, reach):
        for d in (1, -1):
            for p in carried[d] + carried[-d]:
                sends = []
                if step == reach - 2 and p in carried[d]:
                    sends.append(push(step, p, d, 2))
                if step < reach - 1:
                    sends.append(push(step, p, d))
                plan.task(f"z{step}{p}{d}", [f"pg_{step}{p}{d}"], sends=sends)
            plan.task(
                f"h{step}{d}",
                [f"pg_{step}{p}{d}" for p in range(4)],
                sends=[hand_over(-d * step)],
            )
    plan.task(
        f"h{reach}",
        [f"pg_{reach}{p}{d}" for d in (1, -1) for p in carried[d]],
        sends=[hand_over(reach)],
    )
    start.append(hand_over(0))
    return start, names


def plan_plane_scatter(plan, total, short, landing, late, first, second, ready):
    place = plan.place
    half = total.shape[2] // 2
    parts = (pl.ds(0, half), pl.ds(half, half))
    far_land, near_land, sum_land = landing

    def view(array, a, b, h=None):
        at = {first: place.at(first, a), second: place.at(second, b)}
        if h is None:
            return array.at[at["x"], at["y"]]
        return array.at[at["x"], at["y"], parts[h]]

    def ref(a, b, h=None):
        return view(total, a, b, h)

    def send(kind, a, b, h, axis, d, dst, array=total, kib=64):
        name = f"rs_{first}{kind}{b}{h}{d}"
        return (name, axis, d, kib, 1, lambda: (view(array, a, b, h), dst()))

    def far(k):
        return [
            send("f", 2, k, h, first, d, lambda h=h: far_land.at[k % RING, parts[h]], short, 32)
            for h, d in ((0, 1), (1, -1))
        ]

    def own(k):
        return [
            send("n", d, k, h, first, d, lambda h=h: near_land.at[k % RING, parts[h]], short, 32)
            for h, d in ((1, 1), (0, -1))
        ]

    def acc(k, more, needs=()):
        def run():
            for h, d in ((0, 1), (1, -1)):
                ref(d, k, h)[...] += far_land[k % RING, parts[h]].astype(jnp.float32)

        sends = [
            send("n", d, k, h, first, d, lambda h=h: sum_land.at[k % RING, parts[h]])
            for h, d in ((0, 1), (1, -1))
        ]
        needs = [f"rs_{first}f{k}{h}{d}" for h, d in ((0, 1), (1, -1))] + list(needs)
        plan.task(f"{first}acc{k}", needs, run, sends + more, cost=0.15)

    plan.task(f"{first}far2", [ready(2, 2)], sends=far(2))
    plan.task(f"{first}own2", [ready(1, 2), ready(-1, 2)], sends=own(2))
    plan.task(f"{first}far1", [ready(2, 1)], sends=far(1))
    everything = [ready(a, b) for a in (0, 1, 2, -1) for b in (0, 1, 2, -1)]
    acc(2, own(1) + far(-1), everything)
    acc(1, own(-1) + far(0))
    acc(-1, own(0))
    acc(0, [])

    def done(k, sends):
        def run():
            ref(0, k)[...] += near_land[k % RING].astype(jnp.float32) + sum_land[k % RING]

        needs = [f"rs_{first}n{k}{h}{d}" for h in (0, 1) for d in (1, -1)]
        plan.task(f"{first}done{k}", needs, run, sends, cost=0.1)

    def hop(kind, b, h, d, slot):
        return send(kind, 0, b, h, second, d, lambda: late.at[slot, parts[h]])

    done(2, [hop("s", 2, 0, 1, 0), hop("s", 2, 1, -1, 0)])
    done(1, [hop("s", 1, 1, 1, 1)])
    done(-1, [hop("s", -1, 0, -1, 2)])
    done(0, [])
    for d, h, slot in ((1, 0, 1), (-1, 1, 2)):

        def run(d=d, h=h):
            ref(0, d, h)[...] += late[0, parts[h]]

        plan.task(
            f"{first}turn{d}",
            [f"rs_{first}s2{h}{d}", f"{first}done{d}"],
            run,
            [hop("t", d, h, d, slot)],
            cost=0.1,
        )
    last = [f"rs_{first}s11{1}", f"rs_{first}s-10{-1}", f"rs_{first}t10{1}", f"rs_{first}t-11{-1}"]
    return last + [f"{first}done0"]


def plan_line_scatter(plan, total, across, short, short_land, landing, rows, ready):
    z_size = plan.place.z_size
    reach = z_size // 2
    quarter = rows // 4
    parts = [pl.ds(k * quarter, quarter) for k in range(4)]
    carried = {1: (0, 1), -1: (2, 3)}
    opening = {reach: 0, reach - 1: 1, 1 - reach: 2}

    def opens(d, q):
        return 0 if q in carried[d] else 1

    def settle(k):
        s = slot_of(k, z_size)
        total[s, 0] += across[s]
        if k in opening:
            short[opening[k]] = total[s, 0].astype(jnp.bfloat16)

    def push(d, q, step):
        k = d * (reach - step)
        s = slot_of(k, z_size)
        lane = 0 if d == 1 else 1
        name = f"rz_{d}{q}{step}"
        if step == opens(d, q):
            number = opening[k if step else reach]
            both = lambda: (short.at[number, parts[q]], short_land.at[lane, parts[q]])
            return (name, "z", d, 32, 2, both)
        both = lambda: (total.at[s, 0, parts[q]], landing.at[lane, step - 1, parts[q]])
        return (name, "z", d, 64, 2, both)

    for k in [reach] + [s for k in range(reach - 1, 0, -1) for s in (k, -k)] + [0]:
        s = slot_of(k, z_size)
        gift = (f"rz_c{s}", "c", 1, 256, 2, lambda s=s: (total.at[s, 1], across.at[s]))
        plan.task(f"gift{s}", [ready(s)], sends=[gift])
        sends = []
        if k == reach:
            sends = [push(d, q, 0) for d in (1, -1) for q in carried[d]]
        elif k == reach - 1:
            sends = [push(1, q, 1) for q in carried[-1]]
        elif k == 1 - reach:
            sends = [push(-1, q, 1) for q in carried[1]]
        plan.task(f"settle{s}", [f"rz_c{s}", f"gift{s}"], lambda k=k: settle(k), sends, cost=0.12)
    for step in range(1, reach):
        for d in (1, -1):
            for q in carried[d] + carried[-d]:
                if step <= opens(d, q):
                    continue
                s = slot_of(d * (reach - step), z_size)

                def run(d=d, q=q, s=s, step=step):
                    lane = 0 if d == 1 else 1
                    if step - 1 == opens(d, q):
                        value = short_land[lane, parts[q]].astype(jnp.float32)
                    else:
                        value = landing[lane, step - 2, parts[q]]
                    total[s, 0, parts[q]] += value

                plan.task(
                    f"rz{d}{q}{step}",
                    [f"rz_{d}{q}{step - 1}", f"settle{s}"],
                    run,
                    [push(d, q, step)],
                    cost=0.06,
                )
    return [f"rz_{d}{q}{reach - 1}" for d in (1, -1) for q in range(4)] + ["settle0"]


def kernel(
    zl_size,
    z_size,
    q_in,
    p_in,
    t_in,
    loss_out,
    qg_out,
    pg_out,
    qb,
    pb,
    tb,
    scores,
    weights,
    targets,
    tops,
    sums,
    hits,
    stats,
    stats_x,
    mid,
    stats_y,
    factor,
    qga,
    qgb,
    qsa,
    qsb,
    pg,
    far_a,
    near_a,
    sum_a,
    far_b,
    near_b,
    sum_b,
    late_a,
    late_b,
    across,
    short_z,
    short_land_z,
    land_z,
    send_sem,
    recv_sem,
):
    rows, width = q_in.shape
    quarter = rows // 4
    group = RING * rows
    columns = 2 * z_size * rows
    place = Place(zl_size, z_size)
    peers = [("x", k) for k in (1, 2, 3)] + [("y", k) for k in (1, 2, 3)]
    peers += [("z", k) for k in (1, 2, z_size - 2, z_size - 1)] + [("c", 1)]
    barrier = pltpu.get_barrier_semaphore()
    for axis, k in peers:
        pl.semaphore_signal(
            barrier,
            inc=1,
            device_id=place.device(axis, k),
            device_id_type=pl.DeviceIdType.MESH,
        )
    qb[place.x, place.y] = q_in[...].astype(jnp.bfloat16)
    pb[0, 0] = p_in[...].astype(jnp.bfloat16)
    mine = t_in[...]
    tb[place.x * RING + place.y] = jnp.broadcast_to(
        jnp.concatenate([mine] * (128 // rows), axis=1), (8, 128)
    )
    pl.semaphore_wait(barrier, len(peers))

    plan = Plan(place, recv_sem, send_sem)

    start_a, wide_a, brings_a = plan_query_gather(plan, qb, "x", "y", (0, 1), quarter)
    start_b, wide_b, brings_b = plan_query_gather(plan, qb, "y", "x", (2, 3), quarter)
    start_p, crossing = plan_passage_gather(plan, pb, quarter)

    def tile():
        return (tb.at[place.x * RING + place.y],) * 2

    def tiles():
        return (tb.at[pl.ds(place.x * RING, RING)],) * 2

    ty = [(f"tg_y{k}", "y", k, 4, 3, tile) for k in (1, 2, 3)]
    tx = [(f"tg_x{k}", "x", k, 16, 3, tiles) for k in (1, 2, 3)]
    plan.task("open", sends=start_p + start_a + start_b + ty + wide_a + wide_b, rank=-1)
    plan.task("ty", [s[0] for s in ty], sends=tx)

    def at_x(a):
        return place.at("x", a)

    groups = ((0, z_size // 2), (z_size // 2, z_size - 1), (z_size - 1, z_size))

    def multiply(a, g):
        first, last = groups[g]
        size = (last - first) * 2 * rows
        queries = qb[at_x(a)].reshape(group, width)
        start = pl.multiple_of(at_x(a) * columns + first * 2 * rows, 2 * rows)
        scores[pl.ds(start, size)] = (
            lax.dot_general(
                pb[first:last].reshape(size, width),
                queries,
                (((1,), (1,)), ((), ())),
                preferred_element_type=jnp.float32,
            )
            * logit_scale
        )

    band = 128
    bands = columns // band

    def find_targets():
        def split(value, size):
            if size & (size - 1):
                return lax.div(value, size), lax.rem(value, size)
            return value >> (size.bit_length() - 1), value & (size - 1)

        value = jnp.concatenate(
            [
                jnp.concatenate([tb[xs * RING + ys, 0:1, 0:rows] for ys in range(RING)], axis=1)
                for xs in range(RING)
            ],
            axis=0,
        )
        value, inside = split(value, rows)
        value, zh = split(value, z_size // zl_size)
        value, core = split(value, 2)
        value, y = split(value, RING)
        x, zl = split(value, zl_size)
        apart = zh * zl_size + zl - place.z
        apart = jnp.where(apart < 0, apart + z_size, apart)
        slot = jnp.where(apart <= z_size // 2, 2 * apart - 1, 2 * (z_size - apart))
        slot = jnp.where(apart == 0, 0, slot)
        local = (slot * 2 + jnp.where(core == place.c, 0, 1)) * rows + inside
        targets[0:RING] = jnp.where((x == place.x) & (y == place.y), local, -1)

    plan.task("targets", [s[0] for s in tx], find_targets, cost=0.2)

    def fold(value, how):
        return how(value.reshape(band // 8, 8, group), axis=0)

    def piece_of(a, b):
        return pl.ds(pl.multiple_of(at_x(a) * columns + b * band, band), band)

    def measure(a, g):
        multiply(a, g)
        target = targets[pl.ds(at_x(a), 1)]
        low, high = (k * 2 * rows // band for k in groups[g])

        def top(b, highest):
            return jnp.maximum(highest, fold(scores[piece_of(a, b)], jnp.max))

        highest = unrolled(low, high, top, jnp.full((8, group), -jnp.inf, jnp.float32))
        highest = jnp.max(highest, axis=0, keepdims=True)

        def terms(b, totals):
            value = scores[piece_of(a, b)]
            spots = lax.broadcasted_iota(jnp.int32, (band, group), 0) + b * band
            hit = jnp.where(spots == target, value, 0.0)
            value = jnp.exp(value - highest)
            scores[piece_of(a, b)] = value
            return totals[0] + fold(value, jnp.sum), totals[1] + fold(hit, jnp.sum)

        zero = jnp.zeros((8, group), jnp.float32)
        total, hit = unrolled(low, high, terms, (zero, zero))
        total = jnp.sum(total, axis=0, keepdims=True)
        tops[pl.ds(g * RING + at_x(a), 1)] = highest
        sums[pl.ds(g * RING + at_x(a), 1)] = highest + jnp.log(total)
        hits[pl.ds(g * RING + at_x(a), 1)] = jnp.sum(hit, axis=0, keepdims=True)

    def arrived(s):
        if s == 0:
            return [crossing_of[s]]
        if s == z_size - 1:
            return [crossing_of[s], f"h{z_size // 2}"]
        k = (s + 1) // 2 * (1 if s % 2 else -1)
        return [crossing_of[s], f"h{abs(k)}{-1 if k > 0 else 1}"]

    crossing_of = {int(name[4:]): name for name in crossing}
    for rank, a in enumerate((0, -1, 1, 2)):
        needs = [n for b in (-1, 0, 1, 2) for n in brings_a.get((a, b), []) + brings_b.get((b, a), [])]
        needs += ["targets"]
        for g, (first, last) in enumerate(groups):
            plan.task(
                f"measure{a}{g}",
                needs + [n for s in range(first, last) for n in arrived(s)],
                lambda a=a, g=g: measure(a, g),
                cost=0.1 + 0.15 * (last - first),
                rank=1 + rank,
            )

    def total_of(pieces):
        highest = functools.reduce(jnp.maximum, pieces)
        return highest + jnp.log(sum(jnp.exp(piece - highest) for piece in pieces))

    def first_part():
        pieces = range(0, 3 * RING, RING)
        stats[0:RING] = total_of([sums[k : k + RING] for k in pieces])
        stats[RING:] = sum(hits[k : k + RING] for k in pieces)

    def half_way():
        pieces = [stats[...]] + [stats_x[k] for k in range(3)]
        mid[0:RING] = total_of([piece[:RING] for piece in pieces])
        mid[RING:] = sum(piece[RING:] for piece in pieces)

    def normalise():
        pieces = [mid[...]] + [stats_y[k] for k in range(3)]
        log_norm = total_of([piece[:RING] for piece in pieces])
        for k in range(0, 3 * RING, RING):
            factor[k : k + RING] = jnp.exp(tops[k : k + RING] - log_norm)
        losses = log_norm - sum(piece[RING:] for piece in pieces)
        line = lax.broadcasted_iota(jnp.int32, losses.shape, 0)
        losses = jnp.sum(jnp.where(line == place.x, losses, 0.0), axis=0, keepdims=True)
        picked = losses[:, :rows]
        for ys in range(1, RING):
            picked = jnp.where(place.y == ys, losses[:, ys * rows : (ys + 1) * rows], picked)
        loss_out[...] = picked

    sx = [(f"st_x{k}", "x", k, 8, 0, lambda k=k: (stats, stats_x.at[k - 1])) for k in (1, 2, 3)]
    sy = [(f"st_y{k}", "y", k, 8, 0, lambda k=k: (mid, stats_y.at[k - 1])) for k in (1, 2, 3)]
    everything = [t[0] for t in plan.tasks]
    plan.task("sx", everything, first_part, sends=sx)
    plan.task("half", [s[0] for s in sx], half_way, sy)
    plan.task("norm", [s[0] for s in sy], normalise)

    def weigh(a, g):
        target = targets[pl.ds(at_x(a), 1)]
        scale = factor[pl.ds(g * RING + at_x(a), 1)]
        lanes = pl.ds(pl.multiple_of(at_x(a) * group, group), group)

        def step(b, carry):
            spots = lax.broadcasted_iota(jnp.int32, (band, group), 0) + b * band
            onehot = jnp.where(spots == target, 1.0, 0.0)
            weights[pl.ds(pl.multiple_of(b * band, band), band), lanes] = (
                (scores[piece_of(a, b)] * scale - onehot) * logit_scale
            ).astype(jnp.bfloat16)
            return carry

        unrolled(*(k * 2 * rows // band for k in groups[g]), step, 0)

    def passage_terms(first, last):
        some = weights[first * 2 * rows : last * 2 * rows]
        queries = qb[...].reshape(RING * group, width)
        pg[first:last] = jnp.dot(some, queries, preferred_element_type=jnp.float32).reshape(
            last - first, 2, rows, width
        )

    def query_terms(a):
        some = weights[:, pl.ds(pl.multiple_of(at_x(a) * group, group), group)]
        part = lax.dot_general(
            some,
            pb[...].reshape(columns, width),
            (((0,), (0,)), ((), ())),
            preferred_element_type=jnp.float32,
        )
        for array, short, lanes in (
            (qga, qsa, slice(0, width // 2)),
            (qgb, qsb, slice(width // 2, width)),
        ):
            some = part[:, lanes].reshape(RING, rows, width // 2)
            array[at_x(a)] = some
            short[at_x(a)] = some.astype(jnp.bfloat16)

    def weights_of(g):
        for a in (2, 1, -1, 0):
            weigh(a, g)

    cut = z_size - 1
    plan.task("weights2", ["norm"], lambda: weights_of(2), cost=0.1)
    plan.task("pterms0", ["weights2"], lambda: passage_terms(cut, z_size), cost=0.4)
    plan.task("weights1", ["pterms0"], lambda: weights_of(1), cost=0.2)
    plan.task("weights0", ["weights1"], lambda: weights_of(0), cost=0.3)
    plan.task("qterms2", ["weights0"], lambda: query_terms(2), cost=0.8, rank=1)
    plan.task("pterms1", ["qterms2"], lambda: passage_terms(z_size - 3, cut), cost=0.5, rank=1)
    plan.task("qterms1", ["pterms1"], lambda: query_terms(1), cost=0.8, rank=2)
    plan.task("qterms-1", ["qterms1"], lambda: query_terms(-1), cost=0.8, rank=2)
    plan.task("pterms2", ["qterms-1"], lambda: passage_terms(0, z_size - 3), cost=1.2, rank=3)
    plan.task("qterms0", ["pterms2"], lambda: query_terms(0), cost=0.8, rank=4)

    def chunk(a):
        return f"qterms{(a + 1) % 4 - 1}"

    landing = (far_a, near_a, sum_a)
    end_a = plan_plane_scatter(plan, qga, qsa, landing, late_a, "x", "y", lambda a, b: chunk(a))
    landing = (far_b, near_b, sum_b)
    end_b = plan_plane_scatter(plan, qgb, qsb, landing, late_b, "y", "x", lambda a, b: chunk(b))
    end_p = plan_line_scatter(
        plan,
        pg,
        across,
        short_z,
        short_land_z,
        land_z,
        rows,
        lambda s: "pterms0" if s >= cut else ("pterms1" if s >= z_size - 3 else "pterms2"),
    )

    def out_a():
        qg_out[:, : width // 2] = qga[place.x, place.y] + late_a[1] + late_a[2]

    def out_b():
        qg_out[:, width // 2 :] = qgb[place.x, place.y] + late_b[1] + late_b[2]

    def out_p():
        last = z_size // 2 - 2
        pg_out[...] = pg[0, 0] + (land_z[0, last] + land_z[1, last])

    plan.task("out_a", end_a, out_a)
    plan.task("out_b", end_b, out_b)
    plan.task("out_p", end_p, out_p)
    plan.run()
    plan.finish(scores, 0)
    plan.finish(scores, 1)
    plan.finish(scores, 2)
    plan.finish(tb, 3, per_kib=4)


def put_out(*refs):
    for source, target in zip(refs[:3], refs[3:]):
        target[...] = source[...]


def body(zl_size, z_size, queries, passages, positives):
    rows, width = queries.shape
    group = RING * rows
    columns = 2 * z_size * rows
    f32, bf16 = jnp.float32, jnp.bfloat16
    reach = z_size // 2
    shapes = (
        jax.ShapeDtypeStruct((1, rows), f32),
        jax.ShapeDtypeStruct((rows, width), f32),
        jax.ShapeDtypeStruct((rows, width), f32),
    )
    landing = [pltpu.VMEM((RING, rows, width // 2), t) for t in (bf16, bf16, f32)]
    results = pl.pallas_call(
        functools.partial(kernel, zl_size, z_size),
        out_shape=shapes,
        in_specs=[pl.BlockSpec(memory_space=pltpu.VMEM)] * 3,
        out_specs=[pl.BlockSpec(memory_space=pltpu.VMEM)] * 3,
        scratch_shapes=[
            pltpu.VMEM((RING, RING, rows, width), bf16),
            pltpu.VMEM((z_size, 2, rows, width), bf16),
            pltpu.VMEM((RING * RING, 8, 128), jnp.int32),
            pltpu.VMEM((RING * columns, group), f32),
            pltpu.VMEM((columns, RING * group), bf16),
            pltpu.VMEM((2 * RING, group), jnp.int32),
            pltpu.VMEM((4 * RING, group), f32),
            pltpu.VMEM((4 * RING, group), f32),
            pltpu.VMEM((4 * RING, group), f32),
            pltpu.VMEM((2 * RING, group), f32),
            pltpu.VMEM((3, 2 * RING, group), f32),
            pltpu.VMEM((2 * RING, group), f32),
            pltpu.VMEM((3, 2 * RING, group), f32),
            pltpu.VMEM((4 * RING, group), f32),
            pltpu.VMEM((RING, RING, rows, width // 2), f32),
            pltpu.VMEM((RING, RING, rows, width // 2), f32),
            pltpu.VMEM((RING, RING, rows, width // 2), bf16),
            pltpu.VMEM((RING, RING, rows, width // 2), bf16),
            pltpu.VMEM((z_size, 2, rows, width), f32),
            *landing,
            *landing,
            pltpu.VMEM((3, rows, width // 2), f32),
            pltpu.VMEM((3, rows, width // 2), f32),
            pltpu.VMEM((z_size, rows, width), f32),
            pltpu.VMEM((3, rows, width), bf16),
            pltpu.VMEM((2, rows, width), bf16),
            pltpu.VMEM((2, reach - 1, rows, width), f32),
            pltpu.SemaphoreType.DMA((4,)),
            pltpu.SemaphoreType.DMA((SIGNALS,)),
        ],
        compiler_params=pltpu.CompilerParams(
            collective_id=0, has_side_effects=True, vmem_limit_bytes=56 * 1024 * 1024
        ),
    )(queries, passages, positives.reshape(1, rows))
    losses, query_grads, passage_grads = pl.pallas_call(
        put_out,
        out_shape=shapes,
        in_specs=[pl.BlockSpec(memory_space=pltpu.VMEM)] * 3,
        out_specs=[pl.BlockSpec(memory_space=pltpu.VMEM)] * 3,
    )(*results)
    return losses.reshape(rows), query_grads, passage_grads


def solution(mesh):
    zl_size, z_hi = 2, mesh.shape["sub"]
    torus = Mesh(mesh.devices.reshape(RING, zl_size, RING, 2, z_hi), AXES)
    return jax.shard_map(
        functools.partial(body, zl_size, zl_size * z_hi),
        mesh=torus,
        in_specs=(P(AXES, None), P(AXES, None), P(AXES)),
        out_specs=(P(AXES), P(AXES, None), P(AXES, None)),
        check_vma=False,
    )
```

```python
import functools

import jax
import jax.numpy as jnp
from jax import lax
from jax.experimental import pallas as pl
from jax.experimental.pallas import tpu as pltpu
from jax.sharding import Mesh
from jax.sharding import PartitionSpec as P

AXES = ("x", "zl", "y", "c", "zh")
RING = 4
logit_scale = 20.0
SIGNALS = 144

WIRE = {"x": 0.022, "y": 0.022, "z": 0.022, "c": 0.0016}
DELAY = {"x": 2.6, "y": 2.6, "z": 1.5, "c": 0.9}


class Place:
    def __init__(self, zl_size, z_size):
        self.x, self.y, self.c = (lax.axis_index(a) for a in ("x", "y", "c"))
        self.zl_size, self.z_size = zl_size, z_size
        self.z = lax.axis_index("zh") * zl_size + lax.axis_index("zl")

    def at(self, axis, offset):
        size = {"x": RING, "y": RING, "z": self.z_size, "c": 2}[axis]
        return lax.rem(getattr(self, axis) + (offset % size), size)

    def device(self, axis, offset):
        place = self.at(axis, offset)
        if axis == "z":
            return {"zl": lax.rem(place, self.zl_size), "zh": lax.div(place, self.zl_size)}
        return {axis: place}


class Plan:
    def __init__(self, place, recv_sem, send_sems):
        self.place, self.recv_sem, self.send_sems = place, recv_sem, send_sems
        self.tasks = []
        self.slots = {}
        self.copies = {}
        self.sent = {}

    def task(self, name, needs=(), run=None, sends=(), cost=0.05, rank=0):
        self.tasks.append((name, tuple(needs), run, tuple(sends), cost, rank))

    def order(self):
        waiting = list(enumerate(self.tasks))
        known, link, now, result = {}, {}, 0.0, []
        while waiting:
            ready = []
            for index, task in waiting:
                if all(n in known for n in task[1]):
                    ready.append((max([known[n] for n in task[1]], default=0.0), task[5], index, task))
            due = [r for r in ready if r[0] <= now]
            pick = min(due, key=lambda r: (r[1], r[2])) if due else min(ready, key=lambda r: r[:3])
            start, _, index, task = pick
            now = max(now, start) + task[4]
            known[task[0]] = now
            for message, axis, offset, kib, _, _ in task[3]:
                if axis in "xy" and offset == 2:
                    for lane in ((axis, 1), (axis, -1)):
                        link[lane] = max(link.get(lane, 0.0), now) + kib * WIRE[axis]
                    known[message] = max(link[axis, 1], link[axis, -1]) + DELAY[axis] + 0.6
                    continue
                far = abs(offset)
                lane = (axis, offset // far)
                link[lane] = max(link.get(lane, 0.0), now) + kib * WIRE[axis] * far
                known[message] = link[lane] + DELAY[axis] + 0.5 * (far - 1)
            waiting = [w for w in waiting if w[0] != index]
            result.append(task)
        return result

    def signal(self, message):
        kind = message.split("_")[0]
        if kind == "rs":
            kind = "qg"
        group = self.slots.setdefault(message.split("_")[0], {})
        number = group.setdefault(message, len(group))
        base = {"qg": 0, "pg": 60, "tg": 96, "st": 102, "rz": 108}[kind]
        return self.recv_sem.at[base + number]

    def run(self):
        got = set()
        for name, needs, run, sends, _, _ in self.order():
            for need in needs:
                if need in self.copies and need not in got:
                    got.add(need)
                    self.copies[need].wait_recv()
            if run is not None:
                run()
            for message, axis, offset, kib, pool, refs in sends:
                src, dst = refs()
                copy = pltpu.make_async_remote_copy(
                    src_ref=src,
                    dst_ref=dst,
                    send_sem=self.send_sems.at[pool],
                    recv_sem=self.signal(message),
                    device_id=self.place.device(axis, offset),
                    device_id_type=pl.DeviceIdType.MESH,
                )
                copy.start()
                self.copies[message] = copy
                self.sent[pool] = self.sent.get(pool, 0) + kib
        missed = set(self.copies) - got
        assert not missed, missed

    def finish(self, ref, pool, per_kib=1):
        dummy = ref.at[pl.ds(0, self.sent[pool] // per_kib)]
        pltpu.make_async_remote_copy(
            src_ref=dummy,
            dst_ref=dummy,
            send_sem=self.send_sems.at[pool],
            recv_sem=self.recv_sem.at[0],
            device_id=self.place.device("c", 1),
            device_id_type=pl.DeviceIdType.MESH,
        ).wait_send()


def unrolled(first, last, step, carry):
    for k in range(first, last):
        carry = step(k, carry)
    return carry


def slot_of(offset, z_size):
    offset = offset % z_size
    if offset == 0:
        return 0
    if offset <= z_size // 2:
        return 2 * offset - 1
    return 2 * (z_size - offset)


def plan_query_gather(plan, qb, first, second, pieces, quarter):
    place = plan.place
    kib = 32
    brings = {}

    def ref(a, b, p):
        at = {first: place.at(first, a), second: place.at(second, b)}
        return qb.at[at["x"], at["y"], pl.ds(p * quarter, quarter)]

    def send(kind, a, b, p, axis, d):
        name = f"qg_{first}{kind}{a}{p}{d}"
        to = (a - d, b) if axis == first else (a, b - d)
        key = ((to[0] + 1) % 4 - 1, (to[1] + 1) % 4 - 1)
        brings.setdefault(key, []).append(name)
        both = lambda: (ref(a, b, p),) * 2
        return name, (name, axis, d, kib, 0, both)

    u, v = pieces
    opening, names = [], {}
    for p in pieces:
        for d in (1, -1):
            names["f", p, d], s = send("f", 0, 0, p, first, d)
            opening.append((s, p, d))
    opening.sort(key=lambda o: (o[1] == u) != (o[2] == 1))
    start = [o[0] for o in opening]

    def wide(a, p):
        result = []
        for d in (1, -1):
            names["w", a, p, d], s = send("w", a, 0, p, second, d)
            result.append(s)
        return result

    for p in pieces:
        names["far", p], s = send("g", 0, 0, p, first, 2)
        start.append(s)
    widest = [s for p in pieces for s in wide(0, p)]
    for p in pieces:
        plan.task(f"{first}f-1{p}", [names["f", p, 1]], sends=wide(-1, p))
        plan.task(f"{first}f1{p}", [names["f", p, -1]], sends=wide(1, p))
    for p in pieces:
        plan.task(f"{first}g{p}", [names["far", p]], sends=wide(2, p))
    for a in (0, -1, 1, 2):
        for p, b, d in ((u, -1, 1), (v, 1, -1)):
            _, s = send("l", a, b, p, second, d)
            plan.task(f"{first}l{a}{p}", [names["w", a, p, d]], sends=[s])
    return start, widest, brings


def plan_passage_gather(plan, pb, quarter):
    z_size = plan.place.z_size
    reach = z_size // 2
    carried = {1: (0, 1), -1: (2, 3)}
    names = []
    start = []

    def ref(offset, p):
        return pb.at[slot_of(offset, z_size), 0, pl.ds(p * quarter, quarter)]

    def push(step, p, d, places=1):
        both = lambda: (ref(-d * step, p), ref(-d * (step + places), p))
        return (f"pg_{step + places}{p}{d}", "z", d * places, 32, 0, both)

    def hand_over(offset):
        s = slot_of(offset, z_size)
        names.append(f"pg_c{s}")
        return (f"pg_c{s}", "c", 1, 128, 0, lambda: (pb.at[s, 0], pb.at[s, 1]))

    for d in (1, -1):
        for p in carried[d] + carried[-d]:
            start.append(push(0, p, d))
    for step in range(1, reach):
        for d in (1, -1):
            for p in carried[d] + carried[-d]:
                sends = []
                if step == reach - 2 and p in carried[d]:
                    sends.append(push(step, p, d, 2))
                if step < reach - 1:
                    sends.append(push(step, p, d))
                plan.task(f"z{step}{p}{d}", [f"pg_{step}{p}{d}"], sends=sends)
            plan.task(
                f"h{step}{d}",
                [f"pg_{step}{p}{d}" for p in range(4)],
                sends=[hand_over(-d * step)],
            )
    plan.task(
        f"h{reach}",
        [f"pg_{reach}{p}{d}" for d in (1, -1) for p in carried[d]],
        sends=[hand_over(reach)],
    )
    start.append(hand_over(0))
    return start, names


def plan_plane_scatter(plan, total, short, landing, late, first, second, ready):
    place = plan.place
    half = total.shape[2] // 2
    parts = (pl.ds(0, half), pl.ds(half, half))
    far_land, near_land, sum_land = landing

    def view(array, a, b, h=None):
        at = {first: place.at(first, a), second: place.at(second, b)}
        if h is None:
            return array.at[at["x"], at["y"]]
        return array.at[at["x"], at["y"], parts[h]]

    def ref(a, b, h=None):
        return view(total, a, b, h)

    def send(kind, a, b, h, axis, d, dst, array=total, kib=64):
        name = f"rs_{first}{kind}{b}{h}{d}"
        return (name, axis, d, kib, 1, lambda: (view(array, a, b, h), dst()))

    def far(k):
        return [
            send("f", 2, k, h, first, d, lambda h=h: far_land.at[k % RING, parts[h]], short, 32)
            for h, d in ((0, 1), (1, -1))
        ]

    def own(k):
        return [
            send("n", d, k, h, first, d, lambda h=h: near_land.at[k % RING, parts[h]], short, 32)
            for h, d in ((1, 1), (0, -1))
        ]

    def acc(k, more, needs=()):
        def run():
            for h, d in ((0, 1), (1, -1)):
                ref(d, k, h)[...] += far_land[k % RING, parts[h]].astype(jnp.float32)

        sends = [
            send("n", d, k, h, first, d, lambda h=h: sum_land.at[k % RING, parts[h]])
            for h, d in ((0, 1), (1, -1))
        ]
        needs = [f"rs_{first}f{k}{h}{d}" for h, d in ((0, 1), (1, -1))] + list(needs)
        plan.task(f"{first}acc{k}", needs, run, sends + more, cost=0.15)

    plan.task(f"{first}far2", [ready(2, 2)], sends=far(2))
    plan.task(f"{first}own2", [ready(1, 2), ready(-1, 2)], sends=own(2))
    plan.task(f"{first}far1", [ready(2, 1)], sends=far(1))
    everything = [ready(a, b) for a in (0, 1, 2, -1) for b in (0, 1, 2, -1)]
    acc(2, own(1) + far(-1), everything)
    acc(1, own(-1) + far(0))
    acc(-1, own(0))
    acc(0, [])

    def done(k, sends):
        def run():
            ref(0, k)[...] += near_land[k % RING].astype(jnp.float32) + sum_land[k % RING]

        needs = [f"rs_{first}n{k}{h}{d}" for h in (0, 1) for d in (1, -1)]
        plan.task(f"{first}done{k}", needs, run, sends, cost=0.1)

    def hop(kind, b, h, d, slot):
        return send(kind, 0, b, h, second, d, lambda: late.at[slot, parts[h]])

    done(2, [hop("s", 2, 0, 1, 0), hop("s", 2, 1, -1, 0)])
    done(1, [hop("s", 1, 1, 1, 1)])
    done(-1, [hop("s", -1, 0, -1, 2)])
    done(0, [])
    for d, h, slot in ((1, 0, 1), (-1, 1, 2)):

        def run(d=d, h=h):
            ref(0, d, h)[...] += late[0, parts[h]]

        plan.task(
            f"{first}turn{d}",
            [f"rs_{first}s2{h}{d}", f"{first}done{d}"],
            run,
            [hop("t", d, h, d, slot)],
            cost=0.1,
        )
    last = [f"rs_{first}s11{1}", f"rs_{first}s-10{-1}", f"rs_{first}t10{1}", f"rs_{first}t-11{-1}"]
    return last + [f"{first}done0"]


def plan_line_scatter(plan, total, across, short, short_land, landing, rows, ready):
    z_size = plan.place.z_size
    reach = z_size // 2
    quarter = rows // 4
    parts = [pl.ds(k * quarter, quarter) for k in range(4)]
    carried = {1: (0, 1), -1: (2, 3)}
    opening = {reach: 0, reach - 1: 1, 1 - reach: 2}

    def opens(d, q):
        return 0 if q in carried[d] else 1

    def settle(k):
        s = slot_of(k, z_size)
        total[s, 0] += across[s]
        if k in opening:
            short[opening[k]] = total[s, 0].astype(jnp.bfloat16)

    def push(d, q, step):
        k = d * (reach - step)
        s = slot_of(k, z_size)
        lane = 0 if d == 1 else 1
        name = f"rz_{d}{q}{step}"
        if step == opens(d, q):
            number = opening[k if step else reach]
            both = lambda: (short.at[number, parts[q]], short_land.at[lane, parts[q]])
            return (name, "z", d, 32, 2, both)
        both = lambda: (total.at[s, 0, parts[q]], landing.at[lane, step - 1, parts[q]])
        return (name, "z", d, 64, 2, both)

    for k in [reach] + [s for k in range(reach - 1, 0, -1) for s in (k, -k)] + [0]:
        s = slot_of(k, z_size)
        gift = (f"rz_c{s}", "c", 1, 256, 2, lambda s=s: (total.at[s, 1], across.at[s]))
        plan.task(f"gift{s}", [ready(s)], sends=[gift])
        sends = []
        if k == reach:
            sends = [push(d, q, 0) for d in (1, -1) for q in carried[d]]
        elif k == reach - 1:
            sends = [push(1, q, 1) for q in carried[-1]]
        elif k == 1 - reach:
            sends = [push(-1, q, 1) for q in carried[1]]
        plan.task(f"settle{s}", [f"rz_c{s}", f"gift{s}"], lambda k=k: settle(k), sends, cost=0.12)
    for step in range(1, reach):
        for d in (1, -1):
            for q in carried[d] + carried[-d]:
                if step <= opens(d, q):
                    continue
                s = slot_of(d * (reach - step), z_size)

                def run(d=d, q=q, s=s, step=step):
                    lane = 0 if d == 1 else 1
                    if step - 1 == opens(d, q):
                        value = short_land[lane, parts[q]].astype(jnp.float32)
                    else:
                        value = landing[lane, step - 2, parts[q]]
                    total[s, 0, parts[q]] += value

                plan.task(
                    f"rz{d}{q}{step}",
                    [f"rz_{d}{q}{step - 1}", f"settle{s}"],
                    run,
                    [push(d, q, step)],
                    cost=0.06,
                )
    return [f"rz_{d}{q}{reach - 1}" for d in (1, -1) for q in range(4)] + ["settle0"]


def kernel(
    zl_size,
    z_size,
    q_in,
    p_in,
    t_in,
    loss_out,
    qg_out,
    pg_out,
    q_own,
    p_own,
    t_own,
    qb,
    pb,
    tb,
    scores,
    weights,
    targets,
    tops,
    sums,
    hits,
    stats,
    stats_x,
    mid,
    stats_y,
    factor,
    qga,
    qgb,
    qsa,
    qsb,
    pg,
    far_a,
    near_a,
    sum_a,
    far_b,
    near_b,
    sum_b,
    late_a,
    late_b,
    across,
    short_z,
    short_land_z,
    land_z,
    read_sem,
    send_sem,
    recv_sem,
):
    rows, width = q_in.shape
    quarter = rows // 4
    group = RING * rows
    columns = 2 * z_size * rows
    place = Place(zl_size, z_size)
    peers = [("x", k) for k in (1, 2, 3)] + [("y", k) for k in (1, 2, 3)]
    peers += [("z", k) for k in (1, 2, z_size - 2, z_size - 1)] + [("c", 1)]
    barrier = pltpu.get_barrier_semaphore()
    for axis, k in peers:
        pl.semaphore_signal(
            barrier,
            inc=1,
            device_id=place.device(axis, k),
            device_id_type=pl.DeviceIdType.MESH,
        )
    reads = [
        pltpu.make_async_copy(source, target, read_sem.at[k])
        for k, (source, target) in enumerate(((p_in, p_own), (q_in, q_own), (t_in, t_own)))
    ]
    for read in reads:
        read.start()
    reads[0].wait()
    pb[0, 0] = p_own[...].astype(jnp.bfloat16)
    reads[1].wait()
    qb[place.x, place.y] = q_own[...].astype(jnp.bfloat16)
    reads[2].wait()
    mine = t_own[...]
    tb[place.x * RING + place.y] = jnp.broadcast_to(
        jnp.concatenate([mine] * (128 // rows), axis=1), (8, 128)
    )
    pl.semaphore_wait(barrier, len(peers))

    plan = Plan(place, recv_sem, send_sem)

    start_a, wide_a, brings_a = plan_query_gather(plan, qb, "x", "y", (0, 1), quarter)
    start_b, wide_b, brings_b = plan_query_gather(plan, qb, "y", "x", (2, 3), quarter)
    start_p, crossing = plan_passage_gather(plan, pb, quarter)

    def tile():
        return (tb.at[place.x * RING + place.y],) * 2

    def tiles():
        return (tb.at[pl.ds(place.x * RING, RING)],) * 2

    ty = [(f"tg_y{k}", "y", k, 4, 3, tile) for k in (1, 2, 3)]
    tx = [(f"tg_x{k}", "x", k, 16, 3, tiles) for k in (1, 2, 3)]
    plan.task("open", sends=ty + start_p + start_a + start_b + wide_a + wide_b, rank=-1)
    plan.task("ty", [s[0] for s in ty], sends=tx, rank=-1)

    def at_x(a):
        return place.at("x", a)

    groups = ((0, z_size // 2), (z_size // 2, z_size - 1), (z_size - 1, z_size))

    def multiply(a, g):
        first, last = groups[g]
        size = (last - first) * 2 * rows
        queries = qb[at_x(a)].reshape(group, width)
        start = pl.multiple_of(at_x(a) * columns + first * 2 * rows, 2 * rows)
        scores[pl.ds(start, size)] = (
            lax.dot_general(
                pb[first:last].reshape(size, width),
                queries,
                (((1,), (1,)), ((), ())),
                preferred_element_type=jnp.float32,
            )
            * logit_scale
        )

    band = 128
    bands = columns // band

    def find_targets():
        def split(value, size):
            if size & (size - 1):
                return lax.div(value, size), lax.rem(value, size)
            return value >> (size.bit_length() - 1), value & (size - 1)

        value = jnp.concatenate(
            [
                jnp.concatenate([tb[xs * RING + ys, 0:1, 0:rows] for ys in range(RING)], axis=1)
                for xs in range(RING)
            ],
            axis=0,
        )
        value, inside = split(value, rows)
        value, zh = split(value, z_size // zl_size)
        value, core = split(value, 2)
        value, y = split(value, RING)
        x, zl = split(value, zl_size)
        apart = zh * zl_size + zl - place.z
        apart = jnp.where(apart < 0, apart + z_size, apart)
        slot = jnp.where(apart <= z_size // 2, 2 * apart - 1, 2 * (z_size - apart))
        slot = jnp.where(apart == 0, 0, slot)
        local = (slot * 2 + jnp.where(core == place.c, 0, 1)) * rows + inside
        targets[0:RING] = jnp.where((x == place.x) & (y == place.y), local, -1)

    plan.task("targets", [s[0] for s in tx], find_targets, cost=0.2)

    def fold(value, how):
        return how(value.reshape(band // 8, 8, group), axis=0)

    def piece_of(a, b):
        return pl.ds(pl.multiple_of(at_x(a) * columns + b * band, band), band)

    def measure(a, g):
        multiply(a, g)
        target = targets[pl.ds(at_x(a), 1)]
        low, high = (k * 2 * rows // band for k in groups[g])

        def top(b, highest):
            return jnp.maximum(highest, fold(scores[piece_of(a, b)], jnp.max))

        highest = unrolled(low, high, top, jnp.full((8, group), -jnp.inf, jnp.float32))
        highest = jnp.max(highest, axis=0, keepdims=True)

        def terms(b, totals):
            value = scores[piece_of(a, b)]
            spots = lax.broadcasted_iota(jnp.int32, (band, group), 0) + b * band
            hit = jnp.where(spots == target, value, 0.0)
            value = jnp.exp(value - highest)
            scores[piece_of(a, b)] = value
            return totals[0] + fold(value, jnp.sum), totals[1] + fold(hit, jnp.sum)

        zero = jnp.zeros((8, group), jnp.float32)
        total, hit = unrolled(low, high, terms, (zero, zero))
        total = jnp.sum(total, axis=0, keepdims=True)
        tops[pl.ds(g * RING + at_x(a), 1)] = highest
        sums[pl.ds(g * RING + at_x(a), 1)] = highest + jnp.log(total)
        hits[pl.ds(g * RING + at_x(a), 1)] = jnp.sum(hit, axis=0, keepdims=True)

    def arrived(s):
        if s == 0:
            return [crossing_of[s]]
        if s == z_size - 1:
            return [crossing_of[s], f"h{z_size // 2}"]
        k = (s + 1) // 2 * (1 if s % 2 else -1)
        return [crossing_of[s], f"h{abs(k)}{-1 if k > 0 else 1}"]

    crossing_of = {int(name[4:]): name for name in crossing}
    for rank, a in enumerate((0, -1, 1, 2)):
        needs = [n for b in (-1, 0, 1, 2) for n in brings_a.get((a, b), []) + brings_b.get((b, a), [])]
        needs += ["targets"]
        for g, (first, last) in enumerate(groups):
            plan.task(
                f"measure{a}{g}",
                needs + [n for s in range(first, last) for n in arrived(s)],
                lambda a=a, g=g: measure(a, g),
                cost=0.1 + 0.15 * (last - first),
                rank=1 + rank,
            )

    def total_of(pieces):
        highest = functools.reduce(jnp.maximum, pieces)
        return highest + jnp.log(sum(jnp.exp(piece - highest) for piece in pieces))

    def first_part():
        pieces = range(0, 3 * RING, RING)
        stats[0:RING] = total_of([sums[k : k + RING] for k in pieces])
        stats[RING:] = sum(hits[k : k + RING] for k in pieces)

    def half_way():
        pieces = [stats[...]] + [stats_x[k] for k in range(3)]
        mid[0:RING] = total_of([piece[:RING] for piece in pieces])
        mid[RING:] = sum(piece[RING:] for piece in pieces)

    def normalise():
        pieces = [mid[...]] + [stats_y[k] for k in range(3)]
        log_norm = total_of([piece[:RING] for piece in pieces])
        for k in range(0, 3 * RING, RING):
            factor[k : k + RING] = jnp.exp(tops[k : k + RING] - log_norm)
        losses = log_norm - sum(piece[RING:] for piece in pieces)
        line = lax.broadcasted_iota(jnp.int32, losses.shape, 0)
        losses = jnp.sum(jnp.where(line == place.x, losses, 0.0), axis=0, keepdims=True)
        picked = losses[:, :rows]
        for ys in range(1, RING):
            picked = jnp.where(place.y == ys, losses[:, ys * rows : (ys + 1) * rows], picked)
        loss_out[...] = picked

    sx = [(f"st_x{k}", "x", k, 8, 0, lambda k=k: (stats, stats_x.at[k - 1])) for k in (1, 2, 3)]
    sy = [(f"st_y{k}", "y", k, 8, 0, lambda k=k: (mid, stats_y.at[k - 1])) for k in (1, 2, 3)]
    everything = [t[0] for t in plan.tasks]
    plan.task("sx", everything, first_part, sends=sx)
    plan.task("half", [s[0] for s in sx], half_way, sy)
    plan.task("norm", [s[0] for s in sy], normalise)

    def weigh(a, g):
        target = targets[pl.ds(at_x(a), 1)]
        scale = factor[pl.ds(g * RING + at_x(a), 1)]
        lanes = pl.ds(pl.multiple_of(at_x(a) * group, group), group)

        def step(b, carry):
            spots = lax.broadcasted_iota(jnp.int32, (band, group), 0) + b * band
            onehot = jnp.where(spots == target, 1.0, 0.0)
            weights[pl.ds(pl.multiple_of(b * band, band), band), lanes] = (
                (scores[piece_of(a, b)] * scale - onehot) * logit_scale
            ).astype(jnp.bfloat16)
            return carry

        unrolled(*(k * 2 * rows // band for k in groups[g]), step, 0)

    def passage_terms(first, last):
        some = weights[first * 2 * rows : last * 2 * rows]
        queries = qb[...].reshape(RING * group, width)
        pg[first:last] = jnp.dot(some, queries, preferred_element_type=jnp.float32).reshape(
            last - first, 2, rows, width
        )

    def query_terms(a):
        some = weights[:, pl.ds(pl.multiple_of(at_x(a) * group, group), group)]
        part = lax.dot_general(
            some,
            pb[...].reshape(columns, width),
            (((0,), (0,)), ((), ())),
            preferred_element_type=jnp.float32,
        )
        for array, short, lanes in (
            (qga, qsa, slice(0, width // 2)),
            (qgb, qsb, slice(width // 2, width)),
        ):
            some = part[:, lanes].reshape(RING, rows, width // 2)
            array[at_x(a)] = some
            short[at_x(a)] = some.astype(jnp.bfloat16)

    def weights_of(g):
        for a in (2, 1, -1, 0):
            weigh(a, g)

    cut = z_size - 1
    plan.task("weights2", ["norm"], lambda: weights_of(2), cost=0.1)
    plan.task("pterms0", ["weights2"], lambda: passage_terms(cut, z_size), cost=0.4)
    plan.task("weights1", ["pterms0"], lambda: weights_of(1), cost=0.2)
    plan.task("weights0", ["weights1"], lambda: weights_of(0), cost=0.3)
    plan.task("qterms2", ["weights0"], lambda: query_terms(2), cost=0.8, rank=1)
    plan.task("pterms1", ["qterms2"], lambda: passage_terms(z_size - 3, cut), cost=0.5, rank=1)
    plan.task("qterms1", ["pterms1"], lambda: query_terms(1), cost=0.8, rank=2)
    plan.task("qterms-1", ["qterms1"], lambda: query_terms(-1), cost=0.8, rank=2)
    plan.task("pterms2", ["qterms-1"], lambda: passage_terms(0, z_size - 3), cost=1.2, rank=3)
    plan.task("qterms0", ["pterms2"], lambda: query_terms(0), cost=0.8, rank=4)

    def chunk(a):
        return f"qterms{(a + 1) % 4 - 1}"

    landing = (far_a, near_a, sum_a)
    end_a = plan_plane_scatter(plan, qga, qsa, landing, late_a, "x", "y", lambda a, b: chunk(a))
    landing = (far_b, near_b, sum_b)
    end_b = plan_plane_scatter(plan, qgb, qsb, landing, late_b, "y", "x", lambda a, b: chunk(b))
    end_p = plan_line_scatter(
        plan,
        pg,
        across,
        short_z,
        short_land_z,
        land_z,
        rows,
        lambda s: "pterms0" if s >= cut else ("pterms1" if s >= z_size - 3 else "pterms2"),
    )

    def out_a():
        qg_out[:, : width // 2] = qga[place.x, place.y] + late_a[1] + late_a[2]

    def out_b():
        qg_out[:, width // 2 :] = qgb[place.x, place.y] + late_b[1] + late_b[2]

    def out_p():
        last = z_size // 2 - 2
        pg_out[...] = pg[0, 0] + (land_z[0, last] + land_z[1, last])

    plan.task("out_a", end_a, out_a)
    plan.task("out_b", end_b, out_b)
    plan.task("out_p", end_p, out_p)
    plan.run()
    plan.finish(scores, 0)
    plan.finish(scores, 1)
    plan.finish(scores, 2)
    plan.finish(tb, 3, per_kib=4)


def put_out(*refs):
    for source, target in zip(refs[:3], refs[3:]):
        target[...] = source[...]


def body(zl_size, z_size, queries, passages, positives):
    rows, width = queries.shape
    group = RING * rows
    columns = 2 * z_size * rows
    f32, bf16 = jnp.float32, jnp.bfloat16
    reach = z_size // 2
    shapes = (
        jax.ShapeDtypeStruct((1, rows), f32),
        jax.ShapeDtypeStruct((rows, width), f32),
        jax.ShapeDtypeStruct((rows, width), f32),
    )
    landing = [pltpu.VMEM((RING, rows, width // 2), t) for t in (bf16, bf16, f32)]
    results = pl.pallas_call(
        functools.partial(kernel, zl_size, z_size),
        out_shape=tuple(pltpu.VMEM(s.shape, s.dtype) for s in shapes),
        in_specs=[pl.BlockSpec(memory_space=pl.ANY)] * 3,
        out_specs=[pl.BlockSpec(memory_space=pltpu.VMEM)] * 3,
        scratch_shapes=[
            pltpu.VMEM((rows, width), f32),
            pltpu.VMEM((rows, width), f32),
            pltpu.VMEM((1, rows), jnp.int32),
            pltpu.VMEM((RING, RING, rows, width), bf16),
            pltpu.VMEM((z_size, 2, rows, width), bf16),
            pltpu.VMEM((RING * RING, 8, 128), jnp.int32),
            pltpu.VMEM((RING * columns, group), f32),
            pltpu.VMEM((columns, RING * group), bf16),
            pltpu.VMEM((2 * RING, group), jnp.int32),
            pltpu.VMEM((4 * RING, group), f32),
            pltpu.VMEM((4 * RING, group), f32),
            pltpu.VMEM((4 * RING, group), f32),
            pltpu.VMEM((2 * RING, group), f32),
            pltpu.VMEM((3, 2 * RING, group), f32),
            pltpu.VMEM((2 * RING, group), f32),
            pltpu.VMEM((3, 2 * RING, group), f32),
            pltpu.VMEM((4 * RING, group), f32),
            pltpu.VMEM((RING, RING, rows, width // 2), f32),
            pltpu.VMEM((RING, RING, rows, width // 2), f32),
            pltpu.VMEM((RING, RING, rows, width // 2), bf16),
            pltpu.VMEM((RING, RING, rows, width // 2), bf16),
            pltpu.VMEM((z_size, 2, rows, width), f32),
            *landing,
            *landing,
            pltpu.VMEM((3, rows, width // 2), f32),
            pltpu.VMEM((3, rows, width // 2), f32),
            pltpu.VMEM((z_size, rows, width), f32),
            pltpu.VMEM((3, rows, width), bf16),
            pltpu.VMEM((2, rows, width), bf16),
            pltpu.VMEM((2, reach - 1, rows, width), f32),
            pltpu.SemaphoreType.DMA((3,)),
            pltpu.SemaphoreType.DMA((4,)),
            pltpu.SemaphoreType.DMA((SIGNALS,)),
        ],
        compiler_params=pltpu.CompilerParams(
            collective_id=0, has_side_effects=True, vmem_limit_bytes=56 * 1024 * 1024
        ),
    )(queries, passages, positives.reshape(1, rows))
    losses, query_grads, passage_grads = pl.pallas_call(
        put_out,
        out_shape=shapes,
        in_specs=[pl.BlockSpec(memory_space=pltpu.VMEM)] * 3,
        out_specs=[pl.BlockSpec(memory_space=pltpu.VMEM)] * 3,
    )(*(pltpu.with_memory_space_constraint(r, pltpu.VMEM) for r in results))
    return losses.reshape(rows), query_grads, passage_grads


def solution(mesh):
    zl_size, z_hi = 2, mesh.shape["sub"]
    torus = Mesh(mesh.devices.reshape(RING, zl_size, RING, 2, z_hi), AXES)
    return jax.shard_map(
        functools.partial(body, zl_size, zl_size * z_hi),
        mesh=torus,
        in_specs=(P(AXES, None), P(AXES, None), P(AXES)),
        out_specs=(P(AXES), P(AXES, None), P(AXES, None)),
        check_vma=False,
    )
```

```python
import functools

import jax
import jax.numpy as jnp
from jax import lax
from jax.experimental import pallas as pl
from jax.experimental.pallas import tpu as pltpu
from jax.sharding import Mesh
from jax.sharding import PartitionSpec as P

AXES = ("x", "zl", "y", "c", "zh")
RING = 4
logit_scale = 20.0
SIGNALS = 160

WIRE = {"x": 0.022, "y": 0.022, "z": 0.022, "c": 0.0016}
DELAY = {"x": 2.6, "y": 2.6, "z": 1.5, "c": 0.9}


class Place:
    def __init__(self, zl_size, z_size):
        self.x, self.y, self.c = (lax.axis_index(a) for a in ("x", "y", "c"))
        self.zl_size, self.z_size = zl_size, z_size
        self.z = lax.axis_index("zh") * zl_size + lax.axis_index("zl")

    def at(self, axis, offset):
        size = {"x": RING, "y": RING, "z": self.z_size, "c": 2}[axis]
        return lax.rem(getattr(self, axis) + (offset % size), size)

    def device(self, axis, offset):
        if axis == "xy":
            return {"x": self.at("x", offset[0]), "y": self.at("y", offset[1])}
        place = self.at(axis, offset)
        if axis == "z":
            return {"zl": lax.rem(place, self.zl_size), "zh": lax.div(place, self.zl_size)}
        return {axis: place}


class Plan:
    def __init__(self, place, recv_sem, send_sems):
        self.place, self.recv_sem, self.send_sems = place, recv_sem, send_sems
        self.tasks = []
        self.slots = {}
        self.copies = {}
        self.sent = {}

    def task(self, name, needs=(), run=None, sends=(), cost=0.05, rank=0):
        self.tasks.append((name, tuple(needs), run, tuple(sends), cost, rank))

    def order(self):
        waiting = list(enumerate(self.tasks))
        known, link, now, result = {}, {}, 0.0, []
        while waiting:
            ready = []
            for index, task in waiting:
                if all(n in known for n in task[1]):
                    ready.append((max([known[n] for n in task[1]], default=0.0), task[5], index, task))
            due = [r for r in ready if r[0] <= now]
            pick = min(due, key=lambda r: (r[1], r[2])) if due else min(ready, key=lambda r: r[:3])
            start, _, index, task = pick
            now = max(now, start) + task[4]
            known[task[0]] = now
            for message, axis, offset, kib, _, _ in task[3]:
                if axis in "xy" and offset == 2:
                    for lane in ((axis, 1), (axis, -1)):
                        link[lane] = max(link.get(lane, 0.0), now) + kib * WIRE[axis]
                    known[message] = max(link[axis, 1], link[axis, -1]) + DELAY[axis] + 0.6
                    continue
                if axis == "xy":
                    known[message] = now + 4.5
                    continue
                far = abs(offset)
                lane = (axis, offset // far)
                link[lane] = max(link.get(lane, 0.0), now) + kib * WIRE[axis] * far
                known[message] = link[lane] + DELAY[axis] + 0.5 * (far - 1)
            waiting = [w for w in waiting if w[0] != index]
            result.append(task)
        return result

    def signal(self, message):
        kind = message.split("_")[0]
        if kind == "rs":
            kind = "qg"
        group = self.slots.setdefault(message.split("_")[0], {})
        number = group.setdefault(message, len(group))
        base = {"qg": 0, "pg": 60, "tg": 96, "ht": 102, "rz": 108, "st": 144}[kind]
        return self.recv_sem.at[base + number]

    def run(self):
        got = set()
        for name, needs, run, sends, _, _ in self.order():
            for need in needs:
                if need in self.copies and need not in got:
                    got.add(need)
                    self.copies[need].wait_recv()
            if run is not None:
                run()
            for message, axis, offset, kib, pool, refs in sends:
                src, dst = refs()
                copy = pltpu.make_async_remote_copy(
                    src_ref=src,
                    dst_ref=dst,
                    send_sem=self.send_sems.at[pool],
                    recv_sem=self.signal(message),
                    device_id=self.place.device(axis, offset),
                    device_id_type=pl.DeviceIdType.MESH,
                )
                copy.start()
                self.copies[message] = copy
                self.sent[pool] = self.sent.get(pool, 0) + kib
        missed = set(self.copies) - got
        assert not missed, missed

    def finish(self, ref, pool, per_kib=1):
        dummy = ref.at[pl.ds(0, self.sent[pool] // per_kib)]
        pltpu.make_async_remote_copy(
            src_ref=dummy,
            dst_ref=dummy,
            send_sem=self.send_sems.at[pool],
            recv_sem=self.recv_sem.at[0],
            device_id=self.place.device("c", 1),
            device_id_type=pl.DeviceIdType.MESH,
        ).wait_send()


def unrolled(first, last, step, carry):
    for k in range(first, last):
        carry = step(k, carry)
    return carry


def slot_of(offset, z_size):
    offset = offset % z_size
    if offset == 0:
        return 0
    if offset <= z_size // 2:
        return 2 * offset - 1
    return 2 * (z_size - offset)


def plan_query_gather(plan, qb, first, second, pieces, quarter):
    place = plan.place
    kib = 32
    brings = {}

    def ref(a, b, p):
        at = {first: place.at(first, a), second: place.at(second, b)}
        return qb.at[at["x"], at["y"], pl.ds(p * quarter, quarter)]

    def send(kind, a, b, p, axis, d):
        name = f"qg_{first}{kind}{a}{p}{d}"
        to = (a - d, b) if axis == first else (a, b - d)
        key = ((to[0] + 1) % 4 - 1, (to[1] + 1) % 4 - 1)
        brings.setdefault(key, []).append(name)
        both = lambda: (ref(a, b, p),) * 2
        return name, (name, axis, d, kib, 0, both)

    u, v = pieces
    opening, names = [], {}
    for p in pieces:
        for d in (1, -1):
            names["f", p, d], s = send("f", 0, 0, p, first, d)
            opening.append((s, p, d))
    opening.sort(key=lambda o: (o[1] == u) != (o[2] == 1))
    start = [o[0] for o in opening]

    def wide(a, p):
        result = []
        for d in (1, -1):
            names["w", a, p, d], s = send("w", a, 0, p, second, d)
            result.append(s)
        return result

    for p in pieces:
        names["far", p], s = send("g", 0, 0, p, first, 2)
        start.append(s)
    widest = [s for p in pieces for s in wide(0, p)]
    for p in pieces:
        plan.task(f"{first}f-1{p}", [names["f", p, 1]], sends=wide(-1, p))
        plan.task(f"{first}f1{p}", [names["f", p, -1]], sends=wide(1, p))
    for p in pieces:
        plan.task(f"{first}g{p}", [names["far", p]], sends=wide(2, p))
    for a in (0, -1, 1, 2):
        for p, b, d in ((u, -1, 1), (v, 1, -1)):
            _, s = send("l", a, b, p, second, d)
            plan.task(f"{first}l{a}{p}", [names["w", a, p, d]], sends=[s])
    return start, widest, brings


def plan_passage_gather(plan, pb, quarter):
    z_size = plan.place.z_size
    reach = z_size // 2
    carried = {1: (0, 1), -1: (2, 3)}
    names = []
    start = []

    def ref(offset, p):
        return pb.at[slot_of(offset, z_size), 0, pl.ds(p * quarter, quarter)]

    def push(step, p, d, places=1):
        both = lambda: (ref(-d * step, p), ref(-d * (step + places), p))
        return (f"pg_{step + places}{p}{d}", "z", d * places, 32, 0, both)

    def hand_over(offset):
        s = slot_of(offset, z_size)
        names.append(f"pg_c{s}")
        return (f"pg_c{s}", "c", 1, 128, 0, lambda: (pb.at[s, 0], pb.at[s, 1]))

    for d in (1, -1):
        for p in carried[d] + carried[-d]:
            start.append(push(0, p, d))
    for step in range(1, reach):
        for d in (1, -1):
            for p in carried[d] + carried[-d]:
                sends = []
                if step == reach - 2 and p in carried[d]:
                    sends.append(push(step, p, d, 2))
                if step < reach - 1:
                    sends.append(push(step, p, d))
                plan.task(f"z{step}{p}{d}", [f"pg_{step}{p}{d}"], sends=sends)
            plan.task(
                f"h{step}{d}",
                [f"pg_{step}{p}{d}" for p in range(4)],
                sends=[hand_over(-d * step)],
            )
    plan.task(
        f"h{reach}",
        [f"pg_{reach}{p}{d}" for d in (1, -1) for p in carried[d]],
        sends=[hand_over(reach)],
    )
    start.append(hand_over(0))
    return start, names


def plan_plane_scatter(plan, total, short, landing, late, first, second, ready):
    place = plan.place
    half = total.shape[2] // 2
    parts = (pl.ds(0, half), pl.ds(half, half))
    far_land, near_land, sum_land = landing

    def view(array, a, b, h=None):
        at = {first: place.at(first, a), second: place.at(second, b)}
        if h is None:
            return array.at[at["x"], at["y"]]
        return array.at[at["x"], at["y"], parts[h]]

    def ref(a, b, h=None):
        return view(total, a, b, h)

    def send(kind, a, b, h, axis, d, dst, array=total, kib=64):
        name = f"rs_{first}{kind}{b}{h}{d}"
        return (name, axis, d, kib, 1, lambda: (view(array, a, b, h), dst()))

    def far(k):
        return [
            send("f", 2, k, h, first, d, lambda h=h: far_land.at[k % RING, parts[h]], short, 32)
            for h, d in ((0, 1), (1, -1))
        ]

    def own(k):
        return [
            send("n", d, k, h, first, d, lambda h=h: near_land.at[k % RING, parts[h]], short, 32)
            for h, d in ((1, 1), (0, -1))
        ]

    def acc(k, more, needs=()):
        def run():
            for h, d in ((0, 1), (1, -1)):
                ref(d, k, h)[...] += far_land[k % RING, parts[h]].astype(jnp.float32)

        sends = [
            send("n", d, k, h, first, d, lambda h=h: sum_land.at[k % RING, parts[h]])
            for h, d in ((0, 1), (1, -1))
        ]
        needs = [f"rs_{first}f{k}{h}{d}" for h, d in ((0, 1), (1, -1))] + list(needs)
        plan.task(f"{first}acc{k}", needs, run, sends + more, cost=0.15)

    plan.task(f"{first}far2", [ready(2, 2)], sends=far(2))
    plan.task(f"{first}own2", [ready(1, 2), ready(-1, 2)], sends=own(2))
    plan.task(f"{first}far1", [ready(2, 1)], sends=far(1))
    everything = [ready(a, b) for a in (0, 1, 2, -1) for b in (0, 1, 2, -1)]
    acc(2, own(1) + far(-1), everything)
    acc(1, own(-1) + far(0))
    acc(-1, own(0))
    acc(0, [])

    def done(k, sends):
        def run():
            ref(0, k)[...] += near_land[k % RING].astype(jnp.float32) + sum_land[k % RING]

        needs = [f"rs_{first}n{k}{h}{d}" for h in (0, 1) for d in (1, -1)]
        plan.task(f"{first}done{k}", needs, run, sends, cost=0.1)

    def hop(kind, b, h, d, slot):
        return send(kind, 0, b, h, second, d, lambda: late.at[slot, parts[h]])

    done(2, [hop("s", 2, 0, 1, 0), hop("s", 2, 1, -1, 0)])
    done(1, [hop("s", 1, 1, 1, 1)])
    done(-1, [hop("s", -1, 0, -1, 2)])
    done(0, [])
    for d, h, slot in ((1, 0, 1), (-1, 1, 2)):

        def run(d=d, h=h):
            ref(0, d, h)[...] += late[0, parts[h]]

        plan.task(
            f"{first}turn{d}",
            [f"rs_{first}s2{h}{d}", f"{first}done{d}"],
            run,
            [hop("t", d, h, d, slot)],
            cost=0.1,
        )
    last = [f"rs_{first}s11{1}", f"rs_{first}s-10{-1}", f"rs_{first}t10{1}", f"rs_{first}t-11{-1}"]
    return last + [f"{first}done0"]


def plan_line_scatter(plan, total, across, short, short_land, landing, rows, ready):
    z_size = plan.place.z_size
    reach = z_size // 2
    quarter = rows // 4
    parts = [pl.ds(k * quarter, quarter) for k in range(4)]
    carried = {1: (0, 1), -1: (2, 3)}
    opening = {reach: 0, reach - 1: 1, 1 - reach: 2}

    def opens(d, q):
        return 0 if q in carried[d] else 1

    def settle(k):
        s = slot_of(k, z_size)
        total[s, 0] += across[s]
        if k in opening:
            short[opening[k]] = total[s, 0].astype(jnp.bfloat16)

    def push(d, q, step):
        k = d * (reach - step)
        s = slot_of(k, z_size)
        lane = 0 if d == 1 else 1
        name = f"rz_{d}{q}{step}"
        if step == opens(d, q):
            number = opening[k if step else reach]
            both = lambda: (short.at[number, parts[q]], short_land.at[lane, parts[q]])
            return (name, "z", d, 32, 2, both)
        both = lambda: (total.at[s, 0, parts[q]], landing.at[lane, step - 1, parts[q]])
        return (name, "z", d, 64, 2, both)

    for k in [reach] + [s for k in range(reach - 1, 0, -1) for s in (k, -k)] + [0]:
        s = slot_of(k, z_size)
        gift = (f"rz_c{s}", "c", 1, 256, 2, lambda s=s: (total.at[s, 1], across.at[s]))
        plan.task(f"gift{s}", [ready(s)], sends=[gift])
        sends = []
        if k == reach:
            sends = [push(d, q, 0) for d in (1, -1) for q in carried[d]]
        elif k == reach - 1:
            sends = [push(1, q, 1) for q in carried[-1]]
        elif k == 1 - reach:
            sends = [push(-1, q, 1) for q in carried[1]]
        plan.task(f"settle{s}", [f"rz_c{s}", f"gift{s}"], lambda k=k: settle(k), sends, cost=0.12)
    for step in range(1, reach):
        for d in (1, -1):
            for q in carried[d] + carried[-d]:
                if step <= opens(d, q):
                    continue
                s = slot_of(d * (reach - step), z_size)

                def run(d=d, q=q, s=s, step=step):
                    lane = 0 if d == 1 else 1
                    if step - 1 == opens(d, q):
                        value = short_land[lane, parts[q]].astype(jnp.float32)
                    else:
                        value = landing[lane, step - 2, parts[q]]
                    total[s, 0, parts[q]] += value

                plan.task(
                    f"rz{d}{q}{step}",
                    [f"rz_{d}{q}{step - 1}", f"settle{s}"],
                    run,
                    [push(d, q, step)],
                    cost=0.06,
                )
    return [f"rz_{d}{q}{reach - 1}" for d in (1, -1) for q in range(4)] + ["settle0"]


def kernel(
    zl_size,
    z_size,
    q_in,
    p_in,
    t_in,
    loss_out,
    qg_out,
    pg_out,
    q_own,
    p_own,
    t_own,
    qb,
    pb,
    tb,
    scores,
    weights,
    targets,
    tops,
    sums,
    hits,
    stats,
    stats_all,
    hit_own,
    hit_x,
    hit_mid,
    hit_y,
    factor,
    norms,
    qga,
    qgb,
    qsa,
    qsb,
    pg,
    far_a,
    near_a,
    sum_a,
    far_b,
    near_b,
    sum_b,
    late_a,
    late_b,
    across,
    short_z,
    short_land_z,
    land_z,
    read_sem,
    send_sem,
    recv_sem,
):
    rows, width = q_in.shape
    quarter = rows // 4
    group = RING * rows
    columns = 2 * z_size * rows
    place = Place(zl_size, z_size)
    peers = [("x", k) for k in (1, 2, 3)] + [("y", k) for k in (1, 2, 3)]
    peers += [("xy", (a, b)) for a in (1, 2, 3) for b in (1, 2, 3)]
    peers += [("z", k) for k in (1, 2, z_size - 2, z_size - 1)] + [("c", 1)]
    barrier = pltpu.get_barrier_semaphore()
    for axis, k in peers:
        pl.semaphore_signal(
            barrier,
            inc=1,
            device_id=place.device(axis, k),
            device_id_type=pl.DeviceIdType.MESH,
        )
    reads = [
        pltpu.make_async_copy(source, target, read_sem.at[k])
        for k, (source, target) in enumerate(((p_in, p_own), (q_in, q_own), (t_in, t_own)))
    ]
    for read in reads:
        read.start()
    reads[0].wait()
    pb[0, 0] = p_own[...].astype(jnp.bfloat16)
    reads[1].wait()
    qb[place.x, place.y] = q_own[...].astype(jnp.bfloat16)
    reads[2].wait()
    mine = t_own[...]
    tb[place.x * RING + place.y] = jnp.broadcast_to(
        jnp.concatenate([mine] * (128 // rows), axis=1), (8, 128)
    )
    pl.semaphore_wait(barrier, len(peers))

    plan = Plan(place, recv_sem, send_sem)

    start_a, wide_a, brings_a = plan_query_gather(plan, qb, "x", "y", (0, 1), quarter)
    start_b, wide_b, brings_b = plan_query_gather(plan, qb, "y", "x", (2, 3), quarter)
    start_p, crossing = plan_passage_gather(plan, pb, quarter)

    def tile():
        return (tb.at[place.x * RING + place.y],) * 2

    def tiles():
        return (tb.at[pl.ds(place.x * RING, RING)],) * 2

    ty = [(f"tg_y{k}", "y", k, 4, 3, tile) for k in (1, 2, 3)]
    tx = [(f"tg_x{k}", "x", k, 16, 3, tiles) for k in (1, 2, 3)]
    plan.task("open", sends=ty + start_p + start_a + start_b + wide_a + wide_b, rank=-1)
    plan.task("ty", [s[0] for s in ty], sends=tx, rank=-1)

    def at_x(a):
        return place.at("x", a)

    groups = ((0, z_size // 2), (z_size // 2, z_size))

    def multiply(a, g):
        first, last = groups[g]
        size = (last - first) * 2 * rows
        queries = qb[at_x(a)].reshape(group, width)
        start = pl.multiple_of(at_x(a) * columns + first * 2 * rows, 2 * rows)
        scores[pl.ds(start, size)] = (
            lax.dot_general(
                pb[first:last].reshape(size, width),
                queries,
                (((1,), (1,)), ((), ())),
                preferred_element_type=jnp.float32,
            )
            * logit_scale
        )

    band = 128
    bands = columns // band

    def find_targets():
        def split(value, size):
            if size & (size - 1):
                return lax.div(value, size), lax.rem(value, size)
            return value >> (size.bit_length() - 1), value & (size - 1)

        value = jnp.concatenate(
            [
                jnp.concatenate([tb[xs * RING + ys, 0:1, 0:rows] for ys in range(RING)], axis=1)
                for xs in range(RING)
            ],
            axis=0,
        )
        value, inside = split(value, rows)
        value, zh = split(value, z_size // zl_size)
        value, core = split(value, 2)
        value, y = split(value, RING)
        x, zl = split(value, zl_size)
        apart = zh * zl_size + zl - place.z
        apart = jnp.where(apart < 0, apart + z_size, apart)
        slot = jnp.where(apart <= z_size // 2, 2 * apart - 1, 2 * (z_size - apart))
        slot = jnp.where(apart == 0, 0, slot)
        local = (slot * 2 + jnp.where(core == place.c, 0, 1)) * rows + inside
        targets[0:RING] = jnp.where((x == place.x) & (y == place.y), local, -1)

    plan.task("targets", [s[0] for s in tx], find_targets, cost=0.2)

    def fold(value, how):
        return how(value.reshape(band // 8, 8, group), axis=0)

    def piece_of(a, b):
        return pl.ds(pl.multiple_of(at_x(a) * columns + b * band, band), band)

    def measure(a, g):
        multiply(a, g)
        target = targets[pl.ds(at_x(a), 1)]
        low, high = (k * 2 * rows // band for k in groups[g])

        def top(b, highest):
            return jnp.maximum(highest, fold(scores[piece_of(a, b)], jnp.max))

        highest = unrolled(low, high, top, jnp.full((8, group), -jnp.inf, jnp.float32))
        highest = jnp.max(highest, axis=0, keepdims=True)

        def terms(b, totals):
            value = scores[piece_of(a, b)]
            spots = lax.broadcasted_iota(jnp.int32, (band, group), 0) + b * band
            hit = jnp.where(spots == target, value, 0.0)
            value = jnp.exp(value - highest)
            scores[piece_of(a, b)] = value
            return totals[0] + fold(value, jnp.sum), totals[1] + fold(hit, jnp.sum)

        zero = jnp.zeros((8, group), jnp.float32)
        total, hit = unrolled(low, high, terms, (zero, zero))
        total = jnp.sum(total, axis=0, keepdims=True)
        tops[pl.ds(g * RING + at_x(a), 1)] = highest
        sums[pl.ds(g * RING + at_x(a), 1)] = highest + jnp.log(total)
        hits[pl.ds(g * RING + at_x(a), 1)] = jnp.sum(hit, axis=0, keepdims=True)

    def arrived(s):
        if s == 0:
            return [crossing_of[s]]
        if s == z_size - 1:
            return [crossing_of[s], f"h{z_size // 2}"]
        k = (s + 1) // 2 * (1 if s % 2 else -1)
        return [crossing_of[s], f"h{abs(k)}{-1 if k > 0 else 1}"]

    crossing_of = {int(name[4:]): name for name in crossing}
    for rank, a in enumerate((0, -1, 1, 2)):
        needs = [n for b in (-1, 0, 1, 2) for n in brings_a.get((a, b), []) + brings_b.get((b, a), [])]
        needs += ["targets"]
        for g, (first, last) in enumerate(groups):
            plan.task(
                f"measure{a}{g}",
                needs + [n for s in range(first, last) for n in arrived(s)],
                lambda a=a, g=g: measure(a, g),
                cost=0.1 + 0.15 * (last - first),
                rank=1 + rank,
            )

    def total_of(pieces):
        highest = functools.reduce(jnp.maximum, pieces)
        return highest + jnp.log(sum(jnp.exp(piece - highest) for piece in pieces))

    def pack(ref, value):
        ref[0:RING] = value[:, : group // 2]
        ref[RING:] = value[:, group // 2 :]

    def unpack(value):
        return jnp.concatenate([value[:RING], value[RING:]], axis=1)

    def first_part():
        pieces = range(0, len(groups) * RING, RING)
        pack(stats, total_of([sums[k : k + RING] for k in pieces]))
        pack(hit_own, sum(hits[k : k + RING] for k in pieces))

    def normalise():
        norms[...] = total_of([stats[...]] + [stats_all[k] for k in range(RING * RING - 1)])
        log_norm = unpack(norms[...])
        for k in range(0, len(groups) * RING, RING):
            factor[k : k + RING] = jnp.exp(tops[k : k + RING] - log_norm)

    def half_way():
        hit_mid[...] = hit_own[...] + sum(hit_x[k] for k in range(3))

    def put_losses():
        losses = unpack(norms[...] - hit_mid[...] - sum(hit_y[k] for k in range(3)))
        line = lax.broadcasted_iota(jnp.int32, losses.shape, 0)
        losses = jnp.sum(jnp.where(line == place.x, losses, 0.0), axis=0, keepdims=True)
        picked = losses[:, :rows]
        for ys in range(1, RING):
            picked = jnp.where(place.y == ys, losses[:, ys * rows : (ys + 1) * rows], picked)
        loss_out[...] = picked

    others = [(a, b) for a in range(RING) for b in range(RING) if a or b]
    others.sort(key=lambda o: -min(o[0], RING - o[0]) - min(o[1], RING - o[1]))
    spread = []
    for number, (a, b) in enumerate(others):
        axis, offset = ("xy", (a, b)) if a and b else (("x", a) if a else ("y", b))
        refs = lambda number=number: (stats, stats_all.at[number])
        spread.append((f"st_{a}{b}", axis, offset, 4, 4, refs))
    hx = [(f"ht_x{k}", "x", k, 4, 0, lambda k=k: (hit_own, hit_x.at[k - 1])) for k in (1, 2, 3)]
    hy = [(f"ht_y{k}", "y", k, 4, 0, lambda k=k: (hit_mid, hit_y.at[k - 1])) for k in (1, 2, 3)]
    everything = [t[0] for t in plan.tasks]
    plan.task("spread", everything, first_part, sends=spread + hx)
    plan.task("norm", [m[0] for m in spread], normalise, rank=-1)
    plan.task("half", ["norm"] + [m[0] for m in hx], half_way, hy, rank=8)
    plan.task("losses", [m[0] for m in hy], put_losses, rank=9)

    def weigh(a, first, last):
        g = 0 if last <= z_size // 2 else 1
        target = targets[pl.ds(at_x(a), 1)]
        scale = factor[pl.ds(g * RING + at_x(a), 1)]
        lanes = pl.ds(pl.multiple_of(at_x(a) * group, group), group)

        def step(b, carry):
            spots = lax.broadcasted_iota(jnp.int32, (band, group), 0) + b * band
            onehot = jnp.where(spots == target, 1.0, 0.0)
            weights[pl.ds(pl.multiple_of(b * band, band), band), lanes] = (
                (scores[piece_of(a, b)] * scale - onehot) * logit_scale
            ).astype(jnp.bfloat16)
            return carry

        unrolled(first * 2 * rows // band, last * 2 * rows // band, step, 0)

    def passage_terms(first, last):
        some = weights[first * 2 * rows : last * 2 * rows]
        queries = qb[...].reshape(RING * group, width)
        pg[first:last] = jnp.dot(some, queries, preferred_element_type=jnp.float32).reshape(
            last - first, 2, rows, width
        )

    def query_terms(a):
        some = weights[:, pl.ds(pl.multiple_of(at_x(a) * group, group), group)]
        part = lax.dot_general(
            some,
            pb[...].reshape(columns, width),
            (((0,), (0,)), ((), ())),
            preferred_element_type=jnp.float32,
        )
        for array, short, lanes in (
            (qga, qsa, slice(0, width // 2)),
            (qgb, qsb, slice(width // 2, width)),
        ):
            some = part[:, lanes].reshape(RING, rows, width // 2)
            array[at_x(a)] = some
            short[at_x(a)] = some.astype(jnp.bfloat16)

    def weights_of(first, last):
        for a in (2, 1, -1, 0):
            weigh(a, first, last)

    cut = z_size - 1
    plan.task("weights2", ["norm"], lambda: weights_of(cut, z_size), cost=0.1)
    plan.task("pterms0", ["weights2"], lambda: passage_terms(cut, z_size), cost=0.4)
    plan.task("weights1", ["pterms0"], lambda: weights_of(z_size // 2, cut), cost=0.2)
    plan.task("weights0", ["weights1"], lambda: weights_of(0, z_size // 2), cost=0.3)
    plan.task("qterms2", ["weights0"], lambda: query_terms(2), cost=0.8, rank=1)
    plan.task("pterms1", ["qterms2"], lambda: passage_terms(z_size - 3, cut), cost=0.5, rank=1)
    plan.task("qterms1", ["pterms1"], lambda: query_terms(1), cost=0.8, rank=2)
    plan.task("qterms-1", ["qterms1"], lambda: query_terms(-1), cost=0.8, rank=2)
    plan.task("pterms2", ["qterms-1"], lambda: passage_terms(0, z_size - 3), cost=1.2, rank=3)
    plan.task("qterms0", ["pterms2"], lambda: query_terms(0), cost=0.8, rank=4)

    def chunk(a):
        return f"qterms{(a + 1) % 4 - 1}"

    landing = (far_a, near_a, sum_a)
    end_a = plan_plane_scatter(plan, qga, qsa, landing, late_a, "x", "y", lambda a, b: chunk(a))
    landing = (far_b, near_b, sum_b)
    end_b = plan_plane_scatter(plan, qgb, qsb, landing, late_b, "y", "x", lambda a, b: chunk(b))
    end_p = plan_line_scatter(
        plan,
        pg,
        across,
        short_z,
        short_land_z,
        land_z,
        rows,
        lambda s: "pterms0" if s >= cut else ("pterms1" if s >= z_size - 3 else "pterms2"),
    )

    def out_a():
        qg_out[:, : width // 2] = qga[place.x, place.y] + late_a[1] + late_a[2]

    def out_b():
        qg_out[:, width // 2 :] = qgb[place.x, place.y] + late_b[1] + late_b[2]

    def out_p():
        last = z_size // 2 - 2
        pg_out[...] = pg[0, 0] + (land_z[0, last] + land_z[1, last])

    plan.task("out_a", end_a, out_a)
    plan.task("out_b", end_b, out_b)
    plan.task("out_p", end_p, out_p)
    plan.run()
    plan.finish(scores, 0)
    plan.finish(scores, 1)
    plan.finish(scores, 2)
    plan.finish(tb, 3, per_kib=4)
    plan.finish(tb, 4, per_kib=4)


def put_out(*refs):
    for source, target in zip(refs[:3], refs[3:]):
        target[...] = source[...]


def body(zl_size, z_size, queries, passages, positives):
    rows, width = queries.shape
    group = RING * rows
    columns = 2 * z_size * rows
    f32, bf16 = jnp.float32, jnp.bfloat16
    reach = z_size // 2
    shapes = (
        jax.ShapeDtypeStruct((1, rows), f32),
        jax.ShapeDtypeStruct((rows, width), f32),
        jax.ShapeDtypeStruct((rows, width), f32),
    )
    line = pltpu.VMEM((2 * RING, group // 2), f32)
    landing = [pltpu.VMEM((RING, rows, width // 2), t) for t in (bf16, bf16, f32)]
    results = pl.pallas_call(
        functools.partial(kernel, zl_size, z_size),
        out_shape=tuple(pltpu.VMEM(s.shape, s.dtype) for s in shapes),
        in_specs=[pl.BlockSpec(memory_space=pl.ANY)] * 3,
        out_specs=[pl.BlockSpec(memory_space=pltpu.VMEM)] * 3,
        scratch_shapes=[
            pltpu.VMEM((rows, width), f32),
            pltpu.VMEM((rows, width), f32),
            pltpu.VMEM((1, rows), jnp.int32),
            pltpu.VMEM((RING, RING, rows, width), bf16),
            pltpu.VMEM((z_size, 2, rows, width), bf16),
            pltpu.VMEM((RING * RING, 8, 128), jnp.int32),
            pltpu.VMEM((RING * columns, group), f32),
            pltpu.VMEM((columns, RING * group), bf16),
            pltpu.VMEM((2 * RING, group), jnp.int32),
            pltpu.VMEM((4 * RING, group), f32),
            pltpu.VMEM((4 * RING, group), f32),
            pltpu.VMEM((4 * RING, group), f32),
            line,
            pltpu.VMEM((RING * RING - 1, 2 * RING, group // 2), f32),
            line,
            pltpu.VMEM((3, 2 * RING, group // 2), f32),
            line,
            pltpu.VMEM((3, 2 * RING, group // 2), f32),
            pltpu.VMEM((4 * RING, group), f32),
            line,
            pltpu.VMEM((RING, RING, rows, width // 2), f32),
            pltpu.VMEM((RING, RING, rows, width // 2), f32),
            pltpu.VMEM((RING, RING, rows, width // 2), bf16),
            pltpu.VMEM((RING, RING, rows, width // 2), bf16),
            pltpu.VMEM((z_size, 2, rows, width), f32),
            *landing,
            *landing,
            pltpu.VMEM((3, rows, width // 2), f32),
            pltpu.VMEM((3, rows, width // 2), f32),
            pltpu.VMEM((z_size, rows, width), f32),
            pltpu.VMEM((3, rows, width), bf16),
            pltpu.VMEM((2, rows, width), bf16),
            pltpu.VMEM((2, reach - 1, rows, width), f32),
            pltpu.SemaphoreType.DMA((3,)),
            pltpu.SemaphoreType.DMA((5,)),
            pltpu.SemaphoreType.DMA((SIGNALS,)),
        ],
        compiler_params=pltpu.CompilerParams(
            collective_id=0, has_side_effects=True, vmem_limit_bytes=56 * 1024 * 1024
        ),
    )(queries, passages, positives.reshape(1, rows))
    losses, query_grads, passage_grads = pl.pallas_call(
        put_out,
        out_shape=shapes,
        in_specs=[pl.BlockSpec(memory_space=pltpu.VMEM)] * 3,
        out_specs=[pl.BlockSpec(memory_space=pltpu.VMEM)] * 3,
    )(*(pltpu.with_memory_space_constraint(r, pltpu.VMEM) for r in results))
    return losses.reshape(rows), query_grads, passage_grads


def solution(mesh):
    zl_size, z_hi = 2, mesh.shape["sub"]
    torus = Mesh(mesh.devices.reshape(RING, zl_size, RING, 2, z_hi), AXES)
    return jax.shard_map(
        functools.partial(body, zl_size, zl_size * z_hi),
        mesh=torus,
        in_specs=(P(AXES, None), P(AXES, None), P(AXES)),
        out_specs=(P(AXES), P(AXES, None), P(AXES, None)),
        check_vma=False,
    )
```

```python
import functools

import jax
import jax.numpy as jnp
from jax import lax
from jax.experimental import pallas as pl
from jax.experimental.pallas import tpu as pltpu
from jax.sharding import Mesh
from jax.sharding import PartitionSpec as P

AXES = ("x", "zl", "y", "c", "zh")
RING = 4
logit_scale = 20.0
SIGNALS = 160

WIRE = {"x": 0.022, "y": 0.022, "z": 0.022, "c": 0.0016}
DELAY = {"x": 2.6, "y": 2.6, "z": 1.5, "c": 0.9}


class Place:
    def __init__(self, zl_size, z_size):
        self.x, self.y, self.c = (lax.axis_index(a) for a in ("x", "y", "c"))
        self.zl_size, self.z_size = zl_size, z_size
        self.z = lax.axis_index("zh") * zl_size + lax.axis_index("zl")

    def at(self, axis, offset):
        size = {"x": RING, "y": RING, "z": self.z_size, "c": 2}[axis]
        return lax.rem(getattr(self, axis) + (offset % size), size)

    def device(self, axis, offset):
        if axis == "xy":
            return {"x": self.at("x", offset[0]), "y": self.at("y", offset[1])}
        place = self.at(axis, offset)
        if axis == "z":
            return {"zl": lax.rem(place, self.zl_size), "zh": lax.div(place, self.zl_size)}
        return {axis: place}


class Plan:
    def __init__(self, place, recv_sem, send_sems):
        self.place, self.recv_sem, self.send_sems = place, recv_sem, send_sems
        self.tasks = []
        self.slots = {}
        self.copies = {}
        self.sent = {}

    def task(self, name, needs=(), run=None, sends=(), cost=0.05, rank=0):
        self.tasks.append((name, tuple(needs), run, tuple(sends), cost, rank))

    def order(self):
        waiting = list(enumerate(self.tasks))
        known, link, now, result = {}, {}, 0.0, []
        while waiting:
            ready = []
            for index, task in waiting:
                if all(n in known for n in task[1]):
                    ready.append((max([known[n] for n in task[1]], default=0.0), task[5], index, task))
            due = [r for r in ready if r[0] <= now]
            pick = min(due, key=lambda r: (r[1], r[2])) if due else min(ready, key=lambda r: r[:3])
            start, _, index, task = pick
            now = max(now, start) + task[4]
            known[task[0]] = now
            for message, axis, offset, kib, _, _ in task[3]:
                if axis in "xy" and offset == 2:
                    for lane in ((axis, 1), (axis, -1)):
                        link[lane] = max(link.get(lane, 0.0), now) + kib * WIRE[axis]
                    known[message] = max(link[axis, 1], link[axis, -1]) + DELAY[axis] + 0.6
                    continue
                if axis == "xy":
                    known[message] = now + 4.5
                    continue
                far = abs(offset)
                lane = (axis, offset // far)
                link[lane] = max(link.get(lane, 0.0), now) + kib * WIRE[axis] * far
                known[message] = link[lane] + DELAY[axis] + 0.5 * (far - 1)
            waiting = [w for w in waiting if w[0] != index]
            result.append(task)
        return result

    def signal(self, message):
        kind = message.split("_")[0]
        if kind == "rs":
            kind = "qg"
        group = self.slots.setdefault(message.split("_")[0], {})
        number = group.setdefault(message, len(group))
        base = {"qg": 0, "pg": 60, "tg": 96, "ht": 102, "rz": 108, "st": 144}[kind]
        return self.recv_sem.at[base + number]

    def run(self):
        got = set()
        for name, needs, run, sends, _, _ in self.order():
            for need in needs:
                if need in self.copies and need not in got:
                    got.add(need)
                    self.copies[need].wait_recv()
            if run is not None:
                run()
            for message, axis, offset, kib, pool, refs in sends:
                src, dst = refs()
                copy = pltpu.make_async_remote_copy(
                    src_ref=src,
                    dst_ref=dst,
                    send_sem=self.send_sems.at[pool],
                    recv_sem=self.signal(message),
                    device_id=self.place.device(axis, offset),
                    device_id_type=pl.DeviceIdType.MESH,
                )
                copy.start()
                self.copies[message] = copy
                self.sent[pool] = self.sent.get(pool, 0) + kib
        missed = set(self.copies) - got
        assert not missed, missed

    def finish(self, ref, pool, per_kib=1):
        dummy = ref.at[pl.ds(0, self.sent[pool] // per_kib)]
        pltpu.make_async_remote_copy(
            src_ref=dummy,
            dst_ref=dummy,
            send_sem=self.send_sems.at[pool],
            recv_sem=self.recv_sem.at[0],
            device_id=self.place.device("c", 1),
            device_id_type=pl.DeviceIdType.MESH,
        ).wait_send()


def unrolled(first, last, step, carry):
    for k in range(first, last):
        carry = step(k, carry)
    return carry


def slot_of(offset, z_size):
    offset = offset % z_size
    if offset == 0:
        return 0
    if offset <= z_size // 2:
        return 2 * offset - 1
    return 2 * (z_size - offset)


def plan_query_gather(plan, qb, first, second, pieces, quarter):
    place = plan.place
    kib = 32
    brings = {}

    def ref(a, b, p):
        at = {first: place.at(first, a), second: place.at(second, b)}
        return qb.at[at["x"], at["y"], pl.ds(p * quarter, quarter)]

    def send(kind, a, b, p, axis, d):
        name = f"qg_{first}{kind}{a}{p}{d}"
        to = (a - d, b) if axis == first else (a, b - d)
        key = ((to[0] + 1) % 4 - 1, (to[1] + 1) % 4 - 1)
        brings.setdefault(key, []).append(name)
        both = lambda: (ref(a, b, p),) * 2
        return name, (name, axis, d, kib, 0, both)

    u, v = pieces
    opening, names = [], {}
    for p in pieces:
        for d in (1, -1):
            names["f", p, d], s = send("f", 0, 0, p, first, d)
            opening.append((s, p, d))
    opening.sort(key=lambda o: (o[1] == u) != (o[2] == 1))
    start = [o[0] for o in opening]

    def wide(a, p):
        result = []
        for d in (1, -1):
            names["w", a, p, d], s = send("w", a, 0, p, second, d)
            result.append(s)
        return result

    for p in pieces:
        names["far", p], s = send("g", 0, 0, p, first, 2)
        start.append(s)
    widest = [s for p in pieces for s in wide(0, p)]
    for p in pieces:
        plan.task(f"{first}f-1{p}", [names["f", p, 1]], sends=wide(-1, p))
        plan.task(f"{first}f1{p}", [names["f", p, -1]], sends=wide(1, p))
    for p in pieces:
        plan.task(f"{first}g{p}", [names["far", p]], sends=wide(2, p))
    for a in (0, -1, 1, 2):
        for p, b, d in ((u, -1, 1), (v, 1, -1)):
            _, s = send("l", a, b, p, second, d)
            plan.task(f"{first}l{a}{p}", [names["w", a, p, d]], sends=[s])
    return start, widest, brings


def plan_passage_gather(plan, pb, quarter):
    z_size = plan.place.z_size
    reach = z_size // 2
    carried = {1: (0, 1), -1: (2, 3)}
    names = []
    start = []

    def ref(offset, p):
        return pb.at[slot_of(offset, z_size), 0, pl.ds(p * quarter, quarter)]

    def push(step, p, d, places=1):
        both = lambda: (ref(-d * step, p), ref(-d * (step + places), p))
        return (f"pg_{step + places}{p}{d}", "z", d * places, 32, 0, both)

    def hand_over(offset):
        s = slot_of(offset, z_size)
        names.append(f"pg_c{s}")
        return (f"pg_c{s}", "c", 1, 128, 0, lambda: (pb.at[s, 0], pb.at[s, 1]))

    for d in (1, -1):
        for p in carried[d] + carried[-d]:
            start.append(push(0, p, d))
    for step in range(1, reach):
        for d in (1, -1):
            for p in carried[d] + carried[-d]:
                sends = []
                if step == reach - 2 and p in carried[d]:
                    sends.append(push(step, p, d, 2))
                if step < reach - 1:
                    sends.append(push(step, p, d))
                plan.task(f"z{step}{p}{d}", [f"pg_{step}{p}{d}"], sends=sends)
            plan.task(
                f"h{step}{d}",
                [f"pg_{step}{p}{d}" for p in range(4)],
                sends=[hand_over(-d * step)],
            )
    plan.task(
        f"h{reach}",
        [f"pg_{reach}{p}{d}" for d in (1, -1) for p in carried[d]],
        sends=[hand_over(reach)],
    )
    start.append(hand_over(0))
    return start, names


def plan_plane_scatter(plan, total, short, landing, late, first, second, ready):
    place = plan.place
    half = total.shape[2] // 2
    parts = (pl.ds(0, half), pl.ds(half, half))
    far_land, near_land, sum_land = landing

    def view(array, a, b, h=None):
        at = {first: place.at(first, a), second: place.at(second, b)}
        if h is None:
            return array.at[at["x"], at["y"]]
        return array.at[at["x"], at["y"], parts[h]]

    def ref(a, b, h=None):
        return view(total, a, b, h)

    def send(kind, a, b, h, axis, d, dst, array=total, kib=64):
        name = f"rs_{first}{kind}{b}{h}{d}"
        return (name, axis, d, kib, 1, lambda: (view(array, a, b, h), dst()))

    def far(k):
        return [
            send("f", 2, k, h, first, d, lambda h=h: far_land.at[k % RING, parts[h]], short, 32)
            for h, d in ((0, 1), (1, -1))
        ]

    def own(k):
        return [
            send("n", d, k, h, first, d, lambda h=h: near_land.at[k % RING, parts[h]], short, 32)
            for h, d in ((1, 1), (0, -1))
        ]

    def acc(k, more, needs=()):
        def run():
            for h, d in ((0, 1), (1, -1)):
                ref(d, k, h)[...] += far_land[k % RING, parts[h]].astype(jnp.float32)

        sends = [
            send("n", d, k, h, first, d, lambda h=h: sum_land.at[k % RING, parts[h]])
            for h, d in ((0, 1), (1, -1))
        ]
        needs = [f"rs_{first}f{k}{h}{d}" for h, d in ((0, 1), (1, -1))] + list(needs)
        plan.task(f"{first}acc{k}", needs, run, sends + more, cost=0.15)

    plan.task(f"{first}far2", [ready(2, 2)], sends=far(2))
    plan.task(f"{first}own2", [ready(1, 2), ready(-1, 2)], sends=own(2))
    plan.task(f"{first}far1", [ready(2, 1)], sends=far(1))
    everything = [ready(a, b) for a in (0, 1, 2, -1) for b in (0, 1, 2, -1)]
    acc(2, own(1) + far(-1), everything)
    acc(1, own(-1) + far(0))
    acc(-1, own(0))
    acc(0, [])

    def done(k, sends):
        def run():
            ref(0, k)[...] += near_land[k % RING].astype(jnp.float32) + sum_land[k % RING]

        needs = [f"rs_{first}n{k}{h}{d}" for h in (0, 1) for d in (1, -1)]
        plan.task(f"{first}done{k}", needs, run, sends, cost=0.1)

    def hop(kind, b, h, d, slot):
        return send(kind, 0, b, h, second, d, lambda: late.at[slot, parts[h]])

    done(2, [hop("s", 2, 0, 1, 0), hop("s", 2, 1, -1, 0)])
    done(1, [hop("s", 1, 1, 1, 1)])
    done(-1, [hop("s", -1, 0, -1, 2)])
    done(0, [])
    for d, h, slot in ((1, 0, 1), (-1, 1, 2)):

        def run(d=d, h=h):
            ref(0, d, h)[...] += late[0, parts[h]]

        plan.task(
            f"{first}turn{d}",
            [f"rs_{first}s2{h}{d}", f"{first}done{d}"],
            run,
            [hop("t", d, h, d, slot)],
            cost=0.1,
        )
    last = [f"rs_{first}s11{1}", f"rs_{first}s-10{-1}", f"rs_{first}t10{1}", f"rs_{first}t-11{-1}"]
    return last + [f"{first}done0"]


def plan_line_scatter(plan, total, across, short, short_land, landing, rows, ready):
    z_size = plan.place.z_size
    reach = z_size // 2
    quarter = rows // 4
    parts = [pl.ds(k * quarter, quarter) for k in range(4)]
    carried = {1: (0, 1), -1: (2, 3)}
    opening = {reach: 0, reach - 1: 1, 1 - reach: 2}

    def opens(d, q):
        return 0 if q in carried[d] else 1

    def settle(k):
        s = slot_of(k, z_size)
        total[s, 0] += across[s]
        if k in opening:
            short[opening[k]] = total[s, 0].astype(jnp.bfloat16)

    def push(d, q, step):
        k = d * (reach - step)
        s = slot_of(k, z_size)
        lane = 0 if d == 1 else 1
        name = f"rz_{d}{q}{step}"
        if step == opens(d, q):
            number = opening[k if step else reach]
            both = lambda: (short.at[number, parts[q]], short_land.at[lane, parts[q]])
            return (name, "z", d, 32, 2, both)
        both = lambda: (total.at[s, 0, parts[q]], landing.at[lane, step - 1, parts[q]])
        return (name, "z", d, 64, 2, both)

    for k in [reach] + [s for k in range(reach - 1, 0, -1) for s in (k, -k)] + [0]:
        s = slot_of(k, z_size)
        gift = (f"rz_c{s}", "c", 1, 256, 2, lambda s=s: (total.at[s, 1], across.at[s]))
        plan.task(f"gift{s}", [ready(s)], sends=[gift])
        sends = []
        if k == reach:
            sends = [push(d, q, 0) for d in (1, -1) for q in carried[d]]
        elif k == reach - 1:
            sends = [push(1, q, 1) for q in carried[-1]]
        elif k == 1 - reach:
            sends = [push(-1, q, 1) for q in carried[1]]
        plan.task(f"settle{s}", [f"rz_c{s}", f"gift{s}"], lambda k=k: settle(k), sends, cost=0.12)
    for step in range(1, reach):
        for d in (1, -1):
            for q in carried[d] + carried[-d]:
                if step <= opens(d, q):
                    continue
                s = slot_of(d * (reach - step), z_size)

                def run(d=d, q=q, s=s, step=step):
                    lane = 0 if d == 1 else 1
                    if step - 1 == opens(d, q):
                        value = short_land[lane, parts[q]].astype(jnp.float32)
                    else:
                        value = landing[lane, step - 2, parts[q]]
                    total[s, 0, parts[q]] += value

                plan.task(
                    f"rz{d}{q}{step}",
                    [f"rz_{d}{q}{step - 1}", f"settle{s}"],
                    run,
                    [push(d, q, step)],
                    cost=0.06,
                )
    return [f"rz_{d}{q}{reach - 1}" for d in (1, -1) for q in range(4)] + ["settle0"]


def kernel(
    zl_size,
    z_size,
    q_in,
    p_in,
    t_in,
    loss_out,
    qg_out,
    pg_out,
    q_own,
    p_own,
    t_own,
    qb,
    pb,
    tb,
    scores,
    weights,
    targets,
    tops,
    sums,
    hits,
    stats,
    stats_all,
    hit_own,
    hit_x,
    hit_mid,
    hit_y,
    factor,
    norms,
    qga,
    qgb,
    qsa,
    qsb,
    pg,
    far_a,
    near_a,
    sum_a,
    far_b,
    near_b,
    sum_b,
    late_a,
    late_b,
    across,
    short_z,
    short_land_z,
    land_z,
    read_sem,
    send_sem,
    recv_sem,
):
    rows, width = q_in.shape
    quarter = rows // 4
    group = RING * rows
    columns = 2 * z_size * rows
    place = Place(zl_size, z_size)
    peers = [("x", k) for k in (1, 2, 3)] + [("y", k) for k in (1, 2, 3)]
    peers += [("xy", (a, b)) for a in (1, 2, 3) for b in (1, 2, 3)]
    peers += [("z", k) for k in (1, 2, z_size - 2, z_size - 1)] + [("c", 1)]
    barrier = pltpu.get_barrier_semaphore()
    for axis, k in peers:
        pl.semaphore_signal(
            barrier,
            inc=1,
            device_id=place.device(axis, k),
            device_id_type=pl.DeviceIdType.MESH,
        )
    reads = [
        pltpu.make_async_copy(source, target, read_sem.at[k])
        for k, (source, target) in enumerate(((p_in, p_own), (q_in, q_own), (t_in, t_own)))
    ]
    for read in reads:
        read.start()
    reads[0].wait()
    pb[0, 0] = p_own[...].astype(jnp.bfloat16)
    reads[1].wait()
    qb[place.x, place.y] = q_own[...].astype(jnp.bfloat16)
    reads[2].wait()
    mine = t_own[...]
    tb[place.x * RING + place.y] = jnp.broadcast_to(
        jnp.concatenate([mine] * (128 // rows), axis=1), (8, 128)
    )
    pl.semaphore_wait(barrier, len(peers))

    plan = Plan(place, recv_sem, send_sem)

    start_a, wide_a, brings_a = plan_query_gather(plan, qb, "x", "y", (0, 1), quarter)
    start_b, wide_b, brings_b = plan_query_gather(plan, qb, "y", "x", (2, 3), quarter)
    start_p, crossing = plan_passage_gather(plan, pb, quarter)

    def tile():
        return (tb.at[place.x * RING + place.y],) * 2

    def tiles():
        return (tb.at[pl.ds(place.x * RING, RING)],) * 2

    ty = [(f"tg_y{k}", "y", k, 4, 3, tile) for k in (1, 2, 3)]
    tx = [(f"tg_x{k}", "x", k, 16, 3, tiles) for k in (1, 2, 3)]
    plan.task("open", sends=ty + start_p + start_a + start_b + wide_a + wide_b, rank=-1)
    plan.task("ty", [s[0] for s in ty], sends=tx, rank=-1)

    def at_x(a):
        return place.at("x", a)

    groups = ((0, z_size // 2), (z_size // 2, z_size))

    def multiply(a, g):
        first, last = groups[g]
        size = (last - first) * 2 * rows
        queries = qb[at_x(a)].reshape(group, width)
        start = pl.multiple_of(at_x(a) * columns + first * 2 * rows, 2 * rows)
        scores[pl.ds(start, size)] = (
            lax.dot_general(
                pb[first:last].reshape(size, width),
                queries,
                (((1,), (1,)), ((), ())),
                preferred_element_type=jnp.float32,
            )
            * logit_scale
        )

    band = 128
    bands = columns // band

    def find_targets():
        def split(value, size):
            if size & (size - 1):
                return lax.div(value, size), lax.rem(value, size)
            return value >> (size.bit_length() - 1), value & (size - 1)

        value = jnp.concatenate(
            [
                jnp.concatenate([tb[xs * RING + ys, 0:1, 0:rows] for ys in range(RING)], axis=1)
                for xs in range(RING)
            ],
            axis=0,
        )
        value, inside = split(value, rows)
        value, zh = split(value, z_size // zl_size)
        value, core = split(value, 2)
        value, y = split(value, RING)
        x, zl = split(value, zl_size)
        apart = zh * zl_size + zl - place.z
        apart = jnp.where(apart < 0, apart + z_size, apart)
        slot = jnp.where(apart <= z_size // 2, 2 * apart - 1, 2 * (z_size - apart))
        slot = jnp.where(apart == 0, 0, slot)
        local = (slot * 2 + jnp.where(core == place.c, 0, 1)) * rows + inside
        targets[0:RING] = jnp.where((x == place.x) & (y == place.y), local, -1)

    plan.task("targets", [s[0] for s in tx], find_targets, cost=0.2)

    def fold(value, how):
        return how(value.reshape(band // 8, 8, group), axis=0)

    def piece_of(a, b):
        return pl.ds(pl.multiple_of(at_x(a) * columns + b * band, band), band)

    def measure(a, g):
        multiply(a, g)
        target = targets[pl.ds(at_x(a), 1)]
        low, high = (k * 2 * rows // band for k in groups[g])

        def top(b, highest):
            return jnp.maximum(highest, fold(scores[piece_of(a, b)], jnp.max))

        highest = unrolled(low, high, top, jnp.full((8, group), -jnp.inf, jnp.float32))
        highest = jnp.max(highest, axis=0, keepdims=True)

        def terms(b, totals):
            value = scores[piece_of(a, b)]
            spots = lax.broadcasted_iota(jnp.int32, (band, group), 0) + b * band
            hit = jnp.where(spots == target, value, 0.0)
            value = jnp.exp(value - highest)
            scores[piece_of(a, b)] = value
            return totals[0] + fold(value, jnp.sum), totals[1] + fold(hit, jnp.sum)

        zero = jnp.zeros((8, group), jnp.float32)
        total, hit = unrolled(low, high, terms, (zero, zero))
        total = jnp.sum(total, axis=0, keepdims=True)
        tops[pl.ds(g * RING + at_x(a), 1)] = highest
        sums[pl.ds(g * RING + at_x(a), 1)] = highest + jnp.log(total)
        hits[pl.ds(g * RING + at_x(a), 1)] = jnp.sum(hit, axis=0, keepdims=True)

    def arrived(s):
        if s == 0:
            return [crossing_of[s]]
        if s == z_size - 1:
            return [crossing_of[s], f"h{z_size // 2}"]
        k = (s + 1) // 2 * (1 if s % 2 else -1)
        return [crossing_of[s], f"h{abs(k)}{-1 if k > 0 else 1}"]

    crossing_of = {int(name[4:]): name for name in crossing}
    for rank, a in enumerate((0, -1, 1, 2)):
        needs = [n for b in (-1, 0, 1, 2) for n in brings_a.get((a, b), []) + brings_b.get((b, a), [])]
        needs += ["targets"]
        for g, (first, last) in enumerate(groups):
            plan.task(
                f"measure{a}{g}",
                needs + [n for s in range(first, last) for n in arrived(s)],
                lambda a=a, g=g: measure(a, g),
                cost=0.1 + 0.15 * (last - first),
                rank=1 + rank,
            )

    def total_of(pieces):
        highest = functools.reduce(jnp.maximum, pieces)
        return highest + jnp.log(sum(jnp.exp(piece - highest) for piece in pieces))

    def pack(ref, value):
        ref[0:RING] = value[:, : group // 2]
        ref[RING:] = value[:, group // 2 :]

    def unpack(value):
        return jnp.concatenate([value[:RING], value[RING:]], axis=1)

    def first_part():
        pieces = range(0, len(groups) * RING, RING)
        pack(stats, total_of([sums[k : k + RING] for k in pieces]))
        pack(hit_own, sum(hits[k : k + RING] for k in pieces))

    def normalise():
        norms[...] = total_of([stats[...]] + [stats_all[k] for k in range(RING * RING - 1)])
        log_norm = unpack(norms[...])
        for k in range(0, len(groups) * RING, RING):
            factor[k : k + RING] = jnp.exp(tops[k : k + RING] - log_norm)

    def half_way():
        hit_mid[...] = hit_own[...] + sum(hit_x[k] for k in range(3))

    def put_losses():
        losses = unpack(norms[...] - hit_mid[...] - sum(hit_y[k] for k in range(3)))
        line = lax.broadcasted_iota(jnp.int32, losses.shape, 0)
        losses = jnp.sum(jnp.where(line == place.x, losses, 0.0), axis=0, keepdims=True)
        picked = losses[:, :rows]
        for ys in range(1, RING):
            picked = jnp.where(place.y == ys, losses[:, ys * rows : (ys + 1) * rows], picked)
        loss_out[...] = picked

    others = [(a, b) for a in range(RING) for b in range(RING) if a or b]
    others.sort(key=lambda o: -min(o[0], RING - o[0]) - min(o[1], RING - o[1]))
    spread = []
    for number, (a, b) in enumerate(others):
        axis, offset = ("xy", (a, b)) if a and b else (("x", a) if a else ("y", b))
        refs = lambda number=number: (stats, stats_all.at[number])
        spread.append((f"st_{a}{b}", axis, offset, 4, 4, refs))
    hx = [(f"ht_x{k}", "x", k, 4, 0, lambda k=k: (hit_own, hit_x.at[k - 1])) for k in (1, 2, 3)]
    hy = [(f"ht_y{k}", "y", k, 4, 0, lambda k=k: (hit_mid, hit_y.at[k - 1])) for k in (1, 2, 3)]
    everything = [t[0] for t in plan.tasks]
    plan.task("spread", everything, first_part, sends=spread + hx)
    plan.task("norm", [m[0] for m in spread], normalise, rank=-1)
    plan.task("half", ["norm"] + [m[0] for m in hx], half_way, hy, rank=8)
    plan.task("losses", [m[0] for m in hy], put_losses, rank=9)

    def weigh(a, first, last):
        g = 0 if last <= z_size // 2 else 1
        target = targets[pl.ds(at_x(a), 1)]
        scale = factor[pl.ds(g * RING + at_x(a), 1)]
        lanes = pl.ds(pl.multiple_of(at_x(a) * group, group), group)

        def step(b, carry):
            spots = lax.broadcasted_iota(jnp.int32, (band, group), 0) + b * band
            onehot = jnp.where(spots == target, 1.0, 0.0)
            weights[pl.ds(pl.multiple_of(b * band, band), band), lanes] = (
                (scores[piece_of(a, b)] * scale - onehot) * logit_scale
            ).astype(jnp.bfloat16)
            return carry

        unrolled(first * 2 * rows // band, last * 2 * rows // band, step, 0)

    def passage_terms(first, last):
        some = weights[first * 2 * rows : last * 2 * rows]
        queries = qb[...].reshape(RING * group, width)
        pg[first:last] = jnp.dot(some, queries, preferred_element_type=jnp.float32).reshape(
            last - first, 2, rows, width
        )

    def query_terms(a):
        some = weights[:, pl.ds(pl.multiple_of(at_x(a) * group, group), group)]
        part = lax.dot_general(
            some,
            pb[...].reshape(columns, width),
            (((0,), (0,)), ((), ())),
            preferred_element_type=jnp.float32,
        )
        for array, short, lanes in (
            (qga, qsa, slice(0, width // 2)),
            (qgb, qsb, slice(width // 2, width)),
        ):
            some = part[:, lanes].reshape(RING, rows, width // 2)
            array[at_x(a)] = some
            short[at_x(a)] = some.astype(jnp.bfloat16)

    def weights_of(first, last):
        for a in (2, 1, -1, 0):
            weigh(a, first, last)

    cut = z_size - 1
    plan.task("weights2", ["norm"], lambda: weights_of(cut, z_size), cost=0.1)
    plan.task("pterms0", ["weights2"], lambda: passage_terms(cut, z_size), cost=0.4)
    plan.task("weights1", ["pterms0"], lambda: weights_of(z_size // 2, cut), cost=0.2)
    plan.task("weights0", ["pterms1"], lambda: weights_of(0, z_size // 2), cost=0.3)
    plan.task("qterms2", ["weights0"], lambda: query_terms(2), cost=0.8, rank=1)
    plan.task("pterms1", ["weights1"], lambda: passage_terms(z_size - 3, cut), cost=0.5, rank=1)
    plan.task("qterms1", ["qterms2"], lambda: query_terms(1), cost=0.8, rank=2)
    plan.task("qterms-1", ["qterms1"], lambda: query_terms(-1), cost=0.8, rank=2)
    plan.task("pterms2", ["qterms-1"], lambda: passage_terms(0, z_size - 3), cost=1.2, rank=3)
    plan.task("qterms0", ["pterms2"], lambda: query_terms(0), cost=0.8, rank=4)

    def chunk(a):
        return f"qterms{(a + 1) % 4 - 1}"

    landing = (far_a, near_a, sum_a)
    end_a = plan_plane_scatter(plan, qga, qsa, landing, late_a, "x", "y", lambda a, b: chunk(a))
    landing = (far_b, near_b, sum_b)
    end_b = plan_plane_scatter(plan, qgb, qsb, landing, late_b, "y", "x", lambda a, b: chunk(b))
    end_p = plan_line_scatter(
        plan,
        pg,
        across,
        short_z,
        short_land_z,
        land_z,
        rows,
        lambda s: "pterms0" if s >= cut else ("pterms1" if s >= z_size - 3 else "pterms2"),
    )

    def out_a():
        qg_out[:, : width // 2] = qga[place.x, place.y] + late_a[1] + late_a[2]

    def out_b():
        qg_out[:, width // 2 :] = qgb[place.x, place.y] + late_b[1] + late_b[2]

    def out_p():
        last = z_size // 2 - 2
        pg_out[...] = pg[0, 0] + (land_z[0, last] + land_z[1, last])

    plan.task("out_a", end_a, out_a)
    plan.task("out_b", end_b, out_b)
    plan.task("out_p", end_p, out_p)
    plan.run()
    plan.finish(scores, 0)
    plan.finish(scores, 1)
    plan.finish(scores, 2)
    plan.finish(tb, 3, per_kib=4)
    plan.finish(tb, 4, per_kib=4)


def put_out(*refs):
    for source, target in zip(refs[:3], refs[3:]):
        target[...] = source[...]


def body(zl_size, z_size, queries, passages, positives):
    rows, width = queries.shape
    group = RING * rows
    columns = 2 * z_size * rows
    f32, bf16 = jnp.float32, jnp.bfloat16
    reach = z_size // 2
    shapes = (
        jax.ShapeDtypeStruct((1, rows), f32),
        jax.ShapeDtypeStruct((rows, width), f32),
        jax.ShapeDtypeStruct((rows, width), f32),
    )
    line = pltpu.VMEM((2 * RING, group // 2), f32)
    landing = [pltpu.VMEM((RING, rows, width // 2), t) for t in (bf16, bf16, f32)]
    results = pl.pallas_call(
        functools.partial(kernel, zl_size, z_size),
        out_shape=tuple(pltpu.VMEM(s.shape, s.dtype) for s in shapes),
        in_specs=[pl.BlockSpec(memory_space=pl.ANY)] * 3,
        out_specs=[pl.BlockSpec(memory_space=pltpu.VMEM)] * 3,
        scratch_shapes=[
            pltpu.VMEM((rows, width), f32),
            pltpu.VMEM((rows, width), f32),
            pltpu.VMEM((1, rows), jnp.int32),
            pltpu.VMEM((RING, RING, rows, width), bf16),
            pltpu.VMEM((z_size, 2, rows, width), bf16),
            pltpu.VMEM((RING * RING, 8, 128), jnp.int32),
            pltpu.VMEM((RING * columns, group), f32),
            pltpu.VMEM((columns, RING * group), bf16),
            pltpu.VMEM((2 * RING, group), jnp.int32),
            pltpu.VMEM((4 * RING, group), f32),
            pltpu.VMEM((4 * RING, group), f32),
            pltpu.VMEM((4 * RING, group), f32),
            line,
            pltpu.VMEM((RING * RING - 1, 2 * RING, group // 2), f32),
            line,
            pltpu.VMEM((3, 2 * RING, group // 2), f32),
            line,
            pltpu.VMEM((3, 2 * RING, group // 2), f32),
            pltpu.VMEM((4 * RING, group), f32),
            line,
            pltpu.VMEM((RING, RING, rows, width // 2), f32),
            pltpu.VMEM((RING, RING, rows, width // 2), f32),
            pltpu.VMEM((RING, RING, rows, width // 2), bf16),
            pltpu.VMEM((RING, RING, rows, width // 2), bf16),
            pltpu.VMEM((z_size, 2, rows, width), f32),
            *landing,
            *landing,
            pltpu.VMEM((3, rows, width // 2), f32),
            pltpu.VMEM((3, rows, width // 2), f32),
            pltpu.VMEM((z_size, rows, width), f32),
            pltpu.VMEM((3, rows, width), bf16),
            pltpu.VMEM((2, rows, width), bf16),
            pltpu.VMEM((2, reach - 1, rows, width), f32),
            pltpu.SemaphoreType.DMA((3,)),
            pltpu.SemaphoreType.DMA((5,)),
            pltpu.SemaphoreType.DMA((SIGNALS,)),
        ],
        compiler_params=pltpu.CompilerParams(
            collective_id=0, has_side_effects=True, vmem_limit_bytes=56 * 1024 * 1024
        ),
    )(queries, passages, positives.reshape(1, rows))
    losses, query_grads, passage_grads = pl.pallas_call(
        put_out,
        out_shape=shapes,
        in_specs=[pl.BlockSpec(memory_space=pltpu.VMEM)] * 3,
        out_specs=[pl.BlockSpec(memory_space=pltpu.VMEM)] * 3,
    )(*(pltpu.with_memory_space_constraint(r, pltpu.VMEM) for r in results))
    return losses.reshape(rows), query_grads, passage_grads


def solution(mesh):
    zl_size, z_hi = 2, mesh.shape["sub"]
    torus = Mesh(mesh.devices.reshape(RING, zl_size, RING, 2, z_hi), AXES)
    return jax.shard_map(
        functools.partial(body, zl_size, zl_size * z_hi),
        mesh=torus,
        in_specs=(P(AXES, None), P(AXES, None), P(AXES)),
        out_specs=(P(AXES), P(AXES, None), P(AXES, None)),
        check_vma=False,
    )
```
